256 devices in a mesh: level: 2 (over core), gx: 4 (over x), yz: 32 (over z, y).
Axes of the slice: x: 4, y: 4, z: 8, core: 2. Of those that a mesh axis runs over, the one named last changes fastest.
Arguments:
- init_field: float32 [128, 512, 256], P('gx', 'yz'), may hold values from -6 to 6
- source: float32 [128, 512, 256], P('gx', 'yz'), may hold values from -4 to 4
- damping: float32 [128, 512, 256], P('gx', 'yz'), may hold values from 0.05 to 2
Outputs:
- final_states: float32 [2, 128, 512, 256], P('level', 'gx', 'yz')
The draws below stay inside these ranges and needn't reach their ends.
All inputs are finite; a program needn't handle non-finite values.
Results may differ from the reference program's by a relative error of at most 0.0001.
Values sent between devices are 32-bit elements; how exact they have to be, the bound alone decides.
A program may use at most 64 MiB of HBM per device.

```python
import math
import jax
import jax.numpy as jnp

STEPS = 3
ITERS = 3
NX = 128
NY = 512
NZ = 256


def block_scale(rng, extent, split, low, high):
    level, own = 1.0, jax.random.fold_in(rng, 6)
    for position, parts in split:
        steps = jnp.exp(jax.random.uniform(jax.random.fold_in(own, position), (parts,), jnp.float32, low / len(split), high / len(split)))
        level = level * jnp.repeat(steps, extent[position] // parts).reshape([-1 if axis == position else 1 for axis in range(len(extent))])
    return level


def noise(stream_key, shape, deviation, most, shards=(), dtype=jnp.bfloat16):
    gain = block_scale(stream_key, shape, shards, -0.22, 0.18) if shards else 1.0
    array = jax.random.normal(stream_key, shape, jnp.float32) * deviation * gain
    return jnp.minimum(jnp.maximum(array, -most), most).astype(dtype)


def setup_inputs(seed: int = 0) -> dict:
    keys = jax.random.split(jax.random.key(seed), 4)
    init_field = noise(keys[0], (NX, NY, NZ), 1.0, 6.0, ((0, 4), (1, 32)), jnp.float32)
    source = noise(keys[1], (NX, NY, NZ), 0.5, 4.0, ((0, 4), (1, 32)), jnp.float32)
    damping = jnp.clip(jnp.exp(math.log(2.0) - 3.6888794 * jax.random.uniform(keys[2], (NX, NY, NZ), jnp.float32) ** block_scale(keys[2], (NX, NY, NZ), ((0, 4), (1, 32)), -0.2, 0.2)), 0.05, 2.0)
    return dict(init_field=init_field, source=source, damping=damping)


diffusion_number = 1.0


def stencil(field, damping):
    padded = jnp.pad(field, 1)
    beside = padded[2:, 1:-1, 1:-1] + padded[:-2, 1:-1, 1:-1]
    beside = beside + padded[1:-1, 2:, 1:-1] + padded[1:-1, :-2, 1:-1]
    beside = beside + padded[1:-1, 1:-1, 2:] + padded[1:-1, 1:-1, :-2]
    return damping * field + diffusion_number * (6.0 * field - beside)


def solve(target, guess, damping):
    answer = guess
    resid = target - (answer + stencil(answer, damping))
    direction = resid
    norm_now = jnp.sum(resid * resid)
    for step in range(ITERS):
        image = direction + stencil(direction, damping)
        alpha = norm_now / jnp.sum(direction * image)
        answer = answer + alpha * direction
        resid = resid - alpha * image
        if step + 1 < ITERS:
            norm_next = jnp.sum(resid * resid)
            direction = resid + (norm_next / norm_now) * direction
            norm_now = norm_next
    return answer


def reference(init_field, source, damping):
    states = [init_field]
    for step in range(STEPS):
        states.append(solve(states[-1] + source, states[-1], damping))
    corrected = init_field
    for step in range(STEPS):
        extra = 0.5 * stencil(states[step + 1] - states[step], damping)
        corrected = solve(corrected + source + extra, corrected, damping)
    return jnp.stack([states[-1], corrected])
```

```python
import functools

import jax
import jax.numpy as jnp
import numpy as np
from jax import lax
from jax.experimental import pallas as pl
from jax.experimental.pallas import tpu as pltpu
from jax.sharding import PartitionSpec as P

STEPS = 3
ITERS = 3
MESH = pl.DeviceIdType.MESH
F32 = jnp.float32

LOW, HIGH = 1.05, 15.0
MID, HALF = (LOW + HIGH) / 2, (HIGH - LOW) / 2
W = 4


def block_polynomial():
    cheb = np.polynomial.chebyshev
    low, high = 2.0, 13.5

    def third(lam):
        x = (lam - (low + high) / 2) / ((high - low) / 2)
        return 4 * x**3 - 3 * x

    nodes = np.cos(np.pi * (np.arange(4) + 0.5) / 4)
    lam = MID + HALF * nodes
    rho = cheb.chebfit(nodes, (1 + (lam - 1) * third(lam) / third(0.0)) / lam, 3)
    return [float(c) for c in cheb.chebmul(rho, [0.0, 1.0])]


PSI = block_polynomial()


def zsum(v0, v1, first, last):
    a0, a1 = pltpu.roll(v0, 1, 1), pltpu.roll(v1, 1, 1)
    b0, b1 = pltpu.roll(v0, 127, 1), pltpu.roll(v1, 127, 1)
    n0 = jnp.where(first, 0.0, a0) + jnp.where(last, b1, b0)
    n1 = jnp.where(first, a0, a1) + jnp.where(last, 0.0, b1)
    return n0, n1


def recurrences(nu):
    c0, c1, c2, c3, c4 = PSI

    def pattern(rows, values):
        j = lax.rem(lax.broadcasted_iota(jnp.int32, (rows, 128), 0), 4)
        out = jnp.full((rows, 128), values[3], F32)
        for q in range(3):
            out = jnp.where(j == q, values[q], out)
        return out

    bands = {
        1: (1.0, 0.5, 0.5, 0.5 / c4),
        -1: (0.0, 0.5, 0.5, 0.5 - 0.5 * c2 / c4),
        0: (0.0, 0.0, 0.0, -0.5 * c3 / c4),
        -2: (0.0, 0.0, 0.0, -0.5 * c1 / c4),
        -3: (0.0, 0.0, 0.0, -0.5 * c0 / c4),
    }
    long = {o: pattern(24, v) for o, v in bands.items()}
    short = {o: pattern(16, v) for o, v in bands.items()}

    def shifted(v, o):
        rows = v.shape[0]
        return v if o % rows == 0 else pltpu.roll(v, o % rows, 0)

    def times(z, shift):
        f, m = z
        fx = sum(shifted(f * short[o], o) for o in bands)
        mx = sum(long[o] * shifted(m, -o) for o in bands)
        return fx + shift * f, mx + shift * m

    def inner(y, z):
        return jnp.sum(y[0] * z[1][:16], axis=0, keepdims=True)

    def axpy(y, s, z):
        return y[0] + s * z[0], y[1] + s * z[1]

    one = jnp.where(lax.broadcasted_iota(jnp.int32, (16, 128), 0) == 0, 1.0, 0.0).astype(F32)
    start = (one, nu)

    def solve(resid, answer):
        direction = resid
        norm = inner(resid, resid)
        for step in range(ITERS):
            image = times(direction, MID / HALF)
            alpha = norm / inner(direction, image)
            answer = axpy(answer, alpha, direction) if answer else (alpha * direction[0], alpha * direction[1])
            if step + 1 < ITERS:
                resid = axpy(resid, -alpha, image)
                following = inner(resid, resid)
                direction = axpy(resid, following / norm, direction)
                norm = following
        return answer

    back = (MID - 1.0) / HALF
    states = [None]
    corrected = None
    for step in range(STEPS):
        state = states[-1]
        resid = axpy(start, -1.0, times(state, back)) if state else start
        states.append(solve(resid, state))
        change = axpy(states[-1], -1.0, state) if state else states[-1]
        inside = axpy(corrected, -0.5, change) if corrected else (-0.5 * change[0], -0.5 * change[1])
        resid = axpy(start, -1.0, times(inside, back))
        corrected = solve(resid, corrected)
    return states[-1][0] * (1.0 / HALF), corrected[0] * (1.0 / HALF)


def kernel(
    init_hbm, source_hbm, damping_hbm, out_hbm,
    vec, diag, init, source, damping, ys, yr, ps, pr, sums, part_a, part_b, mine, theirs,
    local_sem, init_send, init_recv, ghost_send, ghost_recv,
    a_send, a_recv, b_send, b_recv, out_sem, out_send, out_recv,
):
    c = lax.axis_index("level")
    gx = lax.axis_index("gx")
    yz = lax.axis_index("yz")
    other = 1 - c
    beyond = lax.rem(gx + 2 * c + 3, 4)
    above, below = lax.rem(yz + 1, 32), lax.rem(yz + 31, 32)
    far, near = (other, beyond, yz), (other, gx, yz)
    up, down = (c, gx, above), (c, gx, below)
    far_up, far_down = (other, beyond, above), (other, beyond, below)
    near_up, near_down = (other, gx, above), (other, gx, below)
    neighbours = (far, near, up, down, far_up, far_down, near_up, near_down)
    y, z = lax.rem(yz, 4), lax.div(yz, 4)
    plane_slot = gx * 8 + c * 4 + y

    def plane_mate(k):
        slot = lax.rem(plane_slot + k, 32)
        return slot, (lax.rem(lax.div(slot, 4), 2), lax.div(slot, 8), z * 4 + lax.rem(slot, 4))

    def line_mate(k):
        slot = lax.rem(z + k, 8)
        return slot, (c, gx, slot * 4 + y)

    barrier = pltpu.get_barrier_semaphore()
    for device in neighbours:
        pl.semaphore_signal(barrier, inc=1, device_id=device, device_id_type=MESH)

    own = pl.ds(c * 16, 16)
    loads = [
        pltpu.make_async_copy(damping_hbm.at[own], damping, local_sem.at[0]),
        pltpu.make_async_copy(init_hbm.at[own], init.at[pl.ds(1, 16)], local_sem.at[1]),
        pltpu.make_async_copy(
            init_hbm.at[pl.ds(16 - c, 1)], init.at[pl.ds(17 - 17 * c, 1)], local_sem.at[2]
        ),
        pltpu.make_async_copy(source_hbm.at[own], source, local_sem.at[3]),
    ]
    for load in loads:
        load.start()

    def greet_plane(k, carry):
        pl.semaphore_signal(barrier, inc=1, device_id=plane_mate(k)[1], device_id_type=MESH)
        return carry

    lax.fori_loop(1, 32, greet_plane, 0)
    for k in range(1, 8):
        pl.semaphore_signal(barrier, inc=1, device_id=line_mate(k)[1], device_id_type=MESH)

    lane = lax.broadcasted_iota(jnp.int32, (24, 128), 1)
    first, last = lane == 0, lane == 127
    row = lax.broadcasted_iota(jnp.int32, (16, 128), 0)
    top, bottom = row == 0, row == 15
    has_low = jnp.where(yz > 0, 1.0, 0.0).astype(F32)
    has_high = jnp.where(yz < 31, 1.0, 0.0).astype(F32)
    x_low = jnp.where(gx + c > 0, 1.0, 0.0).astype(F32)
    x_high = jnp.where(gx + c < 4, 1.0, 0.0).astype(F32)
    ghost_row = lax.broadcasted_iota(jnp.int32, (8, 128), 0)
    inside = jnp.where(ghost_row < 4, has_high, has_low)

    def send(src, dst, sends, recvs, device):
        copy = pltpu.make_async_remote_copy(
            src_ref=src, dst_ref=dst, send_sem=sends, recv_sem=recvs,
            device_id=device, device_id_type=MESH,
        )
        copy.start()
        return copy

    def exchange(e, ref):
        out, into = ys.at[e], yr.at[e]
        rows = pl.ds(0, 16)
        plan = (
            (out.at[1], into.at[0, pl.ds(4, 16)], up),
            (out.at[0], into.at[1, pl.ds(4, 16)], down),
            (ref.at[pl.ds(4 + 12 * c, 4), rows], ref.at[pl.ds(20 - 20 * c, 4), rows], far),
            (ref.at[pl.ds(16 - 12 * c, 4), rows], ref.at[pl.ds(20 * c, 4), rows], near),
            (out.at[1, pl.ds(13 * c, 3)], into.at[0, pl.ds(20 - 19 * c, 3)], far_up),
            (out.at[0, pl.ds(13 * c, 3)], into.at[1, pl.ds(20 - 19 * c, 3)], far_down),
            (out.at[1, pl.ds(13 - 13 * c, 3)], into.at[0, pl.ds(1 + 19 * c, 3)], near_up),
            (out.at[0, pl.ds(13 - 13 * c, 3)], into.at[1, pl.ds(1 + 19 * c, 3)], near_down),
        )
        return [
            send(src, dst, ghost_send.at[e, i], ghost_recv.at[e, i], device)
            for i, (src, dst, device) in enumerate(plan)
        ]

    def pack(e, x, own_rows):
        ys[e, 0, x] = own_rows[0:4]
        ys[e, 1, x] = own_rows[12:16]

    loads[0].wait()
    loads[1].wait()

    def prepare(x, carry):
        d = (damping[x] + (7.0 - MID)) * (2.0 / HALF)
        diag[x + 4, 0:16] = d
        pack(0, x, d)
        v = init[x + 1]
        ps[0, x] = v[0:1]
        ps[1, x] = v[15:16]
        return carry

    lax.fori_loop(0, 16, prepare, 0)
    loads[2].wait()
    loads[3].wait()
    pl.semaphore_wait(barrier, 46)
    first_sends = [
        send(ps.at[1], pr.at[0], init_send.at[0], init_recv.at[0], up),
        send(ps.at[0], pr.at[1], init_send.at[1], init_recv.at[1], down),
        send(
            init.at[pl.ds(1 + 15 * c, 1)], init.at[pl.ds(17 - 17 * c, 1)],
            init_send.at[2], init_recv.at[2], far,
        ),
    ]
    exchanges = [exchange(0, diag)]

    for copy in first_sends:
        copy.wait_recv()
    init[0] = init[0] * x_low
    init[17] = init[17] * x_high

    def first_vector(x, carry):
        halves = [init[x + 1, :, 0:128], init[x + 1, :, 128:256]]
        along_z = zsum(*halves, first[:16], last[:16])
        done = []
        for h, v in enumerate(halves):
            s = slice(128 * h, 128 * h + 128)
            low = jnp.where(top, pr[0, x, :, s] * has_low, pltpu.roll(v, 1, 0))
            high = jnp.where(bottom, pr[1, x, :, s] * has_high, pltpu.roll(v, 15, 0))
            total = along_z[h] + low + high + init[x, :, s] + init[x + 2, :, s]
            done.append(source[x, :, s] - ((damping[x, :, s] + 6.0) * v - total))
        w = jnp.concatenate(done, axis=1)
        vec[0, x + 4, 0:16] = w
        pack(1, x, w)
        return carry

    lax.fori_loop(0, 16, first_vector, 0)
    exchanges.append(exchange(1, vec.at[0]))

    def merge(e, ref, masked):
        for copy in exchanges[e]:
            copy.wait_recv()

        def ghosts(x, carry):
            tile = jnp.concatenate([yr[e, 1, x], yr[e, 0, x]], axis=0)
            if masked:
                edge = jnp.where(x < 4, x_low, jnp.where(x >= 20, x_high, 1.0))
                keep = inside * edge
                tile = tile * jnp.concatenate([keep, keep], axis=1)
            ref[x, 16:24] = tile
            return carry

        lax.fori_loop(0, 24, ghosts, 0)
        if masked:
            for x in range(4):
                ref[x, 0:16] = ref[x, 0:16] * x_low
                ref[20 + x, 0:16] = ref[20 + x, 0:16] * x_high

    merge(0, diag, False)
    for block in range(3):
        base = 4 * block
        merge(block + 1, vec.at[base], True)
        for j in range(1, 5):
            source_k = base + j - 1

            def plane(x, j=j, source_k=source_k):
                halves = [vec[source_k, x, :, 0:128], vec[source_k, x, :, 128:256]]
                along_z = zsum(*halves, first, last)
                done = []
                for h, v in enumerate(halves):
                    s = slice(128 * h, 128 * h + 128)
                    total = along_z[h] + pltpu.roll(v, 1, 0) + pltpu.roll(v, 23, 0)
                    total = total + (vec[source_k, x - 1, :, s] + vec[source_k, x + 1, :, s])
                    t = diag[x, :, s] * v - total * (2.0 / HALF)
                    done.append(0.5 * t if j == 1 else t - vec[source_k - 1, x, :, s])
                return done

            if j < 4:

                def body(x, carry, j=j, plane=plane):
                    edge = jnp.where(x < 4, x_low, jnp.where(x >= 20, x_high, 1.0))
                    keep = inside * edge
                    for h, t in enumerate(plane(x)):
                        s = slice(128 * h, 128 * h + 128)
                        vec[base + j, x, 0:16, s] = t[0:16] * edge
                        vec[base + j, x, 16:24, s] = t[16:24] * keep
                    return carry

                lax.fori_loop(j, 24 - j, body, 0)
            else:

                def body(x, carry, plane=plane):
                    done = []
                    for h, t in enumerate(plane(x + 4)):
                        s = slice(128 * h, 128 * h + 128)
                        total = PSI[4] * t[0:16]
                        for q in range(4):
                            total = total + PSI[q] * vec[base + q, x + 4, 0:16, s]
                        done.append(total)
                    total = jnp.concatenate(done, axis=1)
                    vec[base + 4, x + 4, 0:16] = total
                    if block < 2:
                        pack(block + 2, x, total)
                    return carry

                lax.fori_loop(0, 16, body, 0)
        if block < 2:
            exchanges.append(exchange(block + 2, vec.at[base + 4]))

        def products(x, carry):
            new = []
            for h in range(4):
                at = (x + 4, slice(8 * (h // 2), 8 * (h // 2) + 8), slice(128 * (h % 2), 128 * (h % 2) + 128))
                v = [vec[(base + q,) + at] for q in range(5)]
                terms = [v[0] * v[q] for q in range(4)] + [v[4] * v[q] for q in range(4)]
                new = [n + t for n, t in zip(new, terms)] if new else terms
            return tuple(a + n for a, n in zip(carry, new))

        totals = lax.fori_loop(0, 16, products, (jnp.zeros((8, 128), F32),) * 8)
        for q, total in enumerate(totals):
            sums[8 * block + q : 8 * block + q + 1] = jnp.sum(total, axis=0, keepdims=True)

    diagonal = lax.broadcasted_iota(jnp.int32, (24, 128), 0) == lane

    def to_row(v):
        return jnp.sum(jnp.where(diagonal, v, 0.0), axis=0, keepdims=True)

    part_a[plane_slot] = to_row(jnp.sum(sums[...], axis=1, keepdims=True))

    def plane_copy(k):
        slot, device = plane_mate(k)
        return slot, pltpu.make_async_remote_copy(
            src_ref=part_a.at[plane_slot], dst_ref=part_a.at[plane_slot],
            send_sem=a_send.at[slot], recv_sem=a_recv.at[plane_slot],
            device_id=device, device_id_type=MESH,
        )

    def plane_wait(k):
        slot, device = plane_mate(k)
        return pltpu.make_async_remote_copy(
            src_ref=part_a.at[slot], dst_ref=part_a.at[slot],
            send_sem=a_send.at[slot], recv_sem=a_recv.at[slot],
            device_id=device, device_id_type=MESH,
        )

    def start_plane(k, carry):
        plane_copy(k)[1].start()
        return carry

    def finish_plane(k, carry):
        plane_wait(k).wait_recv()
        return carry

    lax.fori_loop(1, 32, start_plane, 0)
    lax.fori_loop(1, 32, finish_plane, 0)
    part_b[z] = jnp.sum(part_a[...], axis=0)
    line = []
    for k in range(1, 8):
        slot, device = line_mate(k)
        copy = pltpu.make_async_remote_copy(
            src_ref=part_b.at[z], dst_ref=part_b.at[z],
            send_sem=b_send.at[slot], recv_sem=b_recv.at[z],
            device_id=device, device_id_type=MESH,
        )
        copy.start()
        line.append((slot, device))
    for slot, device in line:
        pltpu.make_async_remote_copy(
            src_ref=part_b.at[slot], dst_ref=part_b.at[slot],
            send_sem=b_send.at[slot], recv_sem=b_recv.at[slot],
            device_id=device, device_id_type=MESH,
        ).wait_recv()
    total = jnp.sum(part_b[...], axis=0)
    nu = jnp.sum(jnp.where(diagonal, total, 0.0), axis=1, keepdims=True)
    predicted, corrected = recurrences(jnp.broadcast_to(nu, (24, 128)))

    upper = jnp.where(c == 1, 1.0, 0.0).astype(F32)
    away = [corrected[k : k + 1] + upper * (predicted[k : k + 1] - corrected[k : k + 1]) for k in range(12)]
    home = [predicted[k : k + 1] + upper * (corrected[k : k + 1] - predicted[k : k + 1]) for k in range(12)]

    def combine(ref, weights):
        def body(x, carry):
            for h in range(2):
                s = slice(128 * h, 128 * h + 128)
                acc = weights[0] * vec[0, x + 4, 0:16, s]
                for k in range(1, 12):
                    acc = acc + weights[k] * vec[k, x + 4, 0:16, s]
                ref[x, :, s] = init[x + 1, :, s] + acc
            return carry

        lax.fori_loop(0, 16, body, 0)

    combine(theirs, away)
    give = send(theirs, out_hbm.at[0, own], out_send, out_recv, near)
    combine(mine, home)
    keep_mine = pltpu.make_async_copy(mine, out_hbm.at[0, own], out_sem)
    keep_mine.start()

    for copy in first_sends:
        copy.wait_send()
    for group in exchanges:
        for copy in group:
            copy.wait_send()

    def drain(k, carry):
        plane_wait(k).wait_send()
        return carry

    lax.fori_loop(1, 32, drain, 0)
    for slot, device in line:
        pltpu.make_async_remote_copy(
            src_ref=part_b.at[z], dst_ref=part_b.at[z],
            send_sem=b_send.at[slot], recv_sem=b_recv.at[slot],
            device_id=device, device_id_type=MESH,
        ).wait_send()
    give.wait_send()
    keep_mine.wait()
    pltpu.make_async_remote_copy(
        src_ref=theirs, dst_ref=out_hbm.at[0, pl.ds(other * 16, 16)],
        send_sem=out_send, recv_sem=out_recv, device_id=near, device_id_type=MESH,
    ).wait_recv()


def per_device(init_field, source, damping):
    anywhere = pl.BlockSpec(memory_space=pl.ANY)
    dma = pltpu.SemaphoreType.DMA
    return pl.pallas_call(
        kernel,
        out_shape=jax.ShapeDtypeStruct((1, 32, 16, 256), F32),
        in_specs=[anywhere] * 3,
        out_specs=anywhere,
        scratch_shapes=[
            pltpu.VMEM((13, 24, 24, 256), F32),
            pltpu.VMEM((24, 24, 256), F32),
            pltpu.VMEM((18, 16, 256), F32),
            pltpu.VMEM((16, 16, 256), F32),
            pltpu.VMEM((16, 16, 256), F32),
            pltpu.VMEM((4, 2, 16, 4, 256), F32),
            pltpu.VMEM((4, 2, 24, 4, 256), F32),
            pltpu.VMEM((2, 16, 1, 256), F32),
            pltpu.VMEM((2, 16, 1, 256), F32),
            pltpu.VMEM((24, 128), F32),
            pltpu.VMEM((32, 1, 128), F32),
            pltpu.VMEM((8, 1, 128), F32),
            pltpu.VMEM((16, 16, 256), F32),
            pltpu.VMEM((16, 16, 256), F32),
            dma((4,)), dma((3,)), dma((3,)), dma((4, 8)), dma((4, 8)),
            dma((32,)), dma((32,)), dma((8,)), dma((8,)), dma, dma, dma,
        ],
        compiler_params=pltpu.CompilerParams(collective_id=0, has_side_effects=True),
        cost_estimate=pl.CostEstimate(flops=50_000_000, bytes_accessed=3_000_000, transcendentals=0),
    )(init_field, source, damping)


def solution(mesh):
    block = P("gx", "yz", None)
    return jax.shard_map(
        per_device,
        mesh=mesh,
        in_specs=(block, block, block),
        out_specs=P("level", "gx", "yz", None),
        check_vma=False,
    )
```

```python
import functools

import jax
import jax.numpy as jnp
import numpy as np
from jax import lax
from jax.experimental import pallas as pl
from jax.experimental.pallas import tpu as pltpu
from jax.sharding import PartitionSpec as P

STEPS = 3
ITERS = 3
MESH = pl.DeviceIdType.MESH
F32 = jnp.float32

LOW, HIGH = 1.05, 15.0
MID, HALF = (LOW + HIGH) / 2, (HIGH - LOW) / 2
W = 4


def block_polynomial():
    cheb = np.polynomial.chebyshev
    low, high = 2.0, 13.5

    def third(lam):
        x = (lam - (low + high) / 2) / ((high - low) / 2)
        return 4 * x**3 - 3 * x

    nodes = np.cos(np.pi * (np.arange(4) + 0.5) / 4)
    lam = MID + HALF * nodes
    rho = cheb.chebfit(nodes, (1 + (lam - 1) * third(lam) / third(0.0)) / lam, 3)
    return [float(c) for c in cheb.chebmul(rho, [0.0, 1.0])]


PSI = block_polynomial()


def planes(start, count, step, body):
    def turn(i, carry):
        for u in range(step):
            body(start + i * step + u)
        return carry

    lax.fori_loop(0, count // step, turn, 0)


def zsum(v0, v1, first, last):
    a0, a1 = pltpu.roll(v0, 1, 1), pltpu.roll(v1, 1, 1)
    b0, b1 = pltpu.roll(v0, 127, 1), pltpu.roll(v1, 127, 1)
    n0 = jnp.where(first, 0.0, a0) + jnp.where(last, b1, b0)
    n1 = jnp.where(first, a0, a1) + jnp.where(last, 0.0, b1)
    return n0, n1


def recurrences(nu):
    c0, c1, c2, c3, c4 = PSI

    def pattern(rows, values):
        j = lax.rem(lax.broadcasted_iota(jnp.int32, (rows, 128), 0), 4)
        out = jnp.full((rows, 128), values[3], F32)
        for q in range(3):
            out = jnp.where(j == q, values[q], out)
        return out

    bands = {
        1: (1.0, 0.5, 0.5, 0.5 / c4),
        -1: (0.0, 0.5, 0.5, 0.5 - 0.5 * c2 / c4),
        0: (0.0, 0.0, 0.0, -0.5 * c3 / c4),
        -2: (0.0, 0.0, 0.0, -0.5 * c1 / c4),
        -3: (0.0, 0.0, 0.0, -0.5 * c0 / c4),
    }
    long = {o: pattern(24, v) for o, v in bands.items()}
    short = {o: pattern(16, v) for o, v in bands.items()}

    def shifted(v, o):
        rows = v.shape[0]
        return v if o % rows == 0 else pltpu.roll(v, o % rows, 0)

    def times(z, shift):
        f, m = z
        fx = sum(shifted(f * short[o], o) for o in bands)
        mx = sum(long[o] * shifted(m, -o) for o in bands)
        return fx + shift * f, mx + shift * m

    def inner(y, z):
        return jnp.sum(y[0] * z[1][:16], axis=0, keepdims=True)

    def axpy(y, s, z):
        return y[0] + s * z[0], y[1] + s * z[1]

    one = jnp.where(lax.broadcasted_iota(jnp.int32, (16, 128), 0) == 0, 1.0, 0.0).astype(F32)
    start = (one, nu)

    def solve(resid, answer):
        direction = resid
        norm = inner(resid, resid)
        for step in range(ITERS):
            image = times(direction, MID / HALF)
            alpha = norm / inner(direction, image)
            answer = axpy(answer, alpha, direction) if answer else (alpha * direction[0], alpha * direction[1])
            if step + 1 < ITERS:
                resid = axpy(resid, -alpha, image)
                following = inner(resid, resid)
                direction = axpy(resid, following / norm, direction)
                norm = following
        return answer

    back = (MID - 1.0) / HALF
    states = [None]
    corrected = None
    for step in range(STEPS):
        state = states[-1]
        resid = axpy(start, -1.0, times(state, back)) if state else start
        states.append(solve(resid, state))
        change = axpy(states[-1], -1.0, state) if state else states[-1]
        inside = axpy(corrected, -0.5, change) if corrected else (-0.5 * change[0], -0.5 * change[1])
        resid = axpy(start, -1.0, times(inside, back))
        corrected = solve(resid, corrected)
    return states[-1][0] * (1.0 / HALF), corrected[0] * (1.0 / HALF)


def kernel(
    init_hbm, source_hbm, damping_hbm, out_hbm,
    vec, diag, init, source, damping, ys, yr, ps, pr, sums, part_a, part_b, mine, theirs,
    local_sem, init_send, init_recv, ghost_send, ghost_recv,
    a_send, a_recv, b_send, b_recv, out_sem, out_send, out_recv,
):
    c = lax.axis_index("level")
    gx = lax.axis_index("gx")
    yz = lax.axis_index("yz")
    other = 1 - c
    beyond = lax.rem(gx + 2 * c + 3, 4)
    above, below = lax.rem(yz + 1, 32), lax.rem(yz + 31, 32)
    far, near = (other, beyond, yz), (other, gx, yz)
    up, down = (c, gx, above), (c, gx, below)
    far_up, far_down = (other, beyond, above), (other, beyond, below)
    near_up, near_down = (other, gx, above), (other, gx, below)
    neighbours = (far, near, up, down, far_up, far_down, near_up, near_down)
    y, z = lax.rem(yz, 4), lax.div(yz, 4)
    plane_slot = gx * 8 + c * 4 + y

    def plane_mate(k):
        slot = lax.rem(plane_slot + k, 32)
        return slot, (lax.rem(lax.div(slot, 4), 2), lax.div(slot, 8), z * 4 + lax.rem(slot, 4))

    def line_mate(k):
        slot = lax.rem(z + k, 8)
        return slot, (c, gx, slot * 4 + y)

    own = pl.ds(c * 16, 16)
    rows = pl.ds(8, 16)
    loads = []
    for h in range(2):
        s = pl.ds(128 * h, 128)
        loads += [
            pltpu.make_async_copy(damping_hbm.at[own, :, s], damping.at[:, h], local_sem.at[h]),
            pltpu.make_async_copy(init_hbm.at[own, :, s], init.at[pl.ds(1, 16), h, rows], local_sem.at[2 + h]),
            pltpu.make_async_copy(
                init_hbm.at[pl.ds(16 - c, 1), :, s], init.at[pl.ds(17 - 17 * c, 1), h, rows], local_sem.at[4 + h]
            ),
            pltpu.make_async_copy(source_hbm.at[own, :, s], source.at[:, h], local_sem.at[6 + h]),
        ]
    for load in loads:
        load.start()

    barrier = pltpu.get_barrier_semaphore()
    for k in range(1, 8):
        pl.semaphore_signal(barrier, inc=1, device_id=line_mate(k)[1], device_id_type=MESH)
    for device in neighbours:
        pl.semaphore_signal(barrier, inc=1, device_id=device, device_id_type=MESH)
    for k in range(1, 32):
        pl.semaphore_signal(barrier, inc=1, device_id=plane_mate(k)[1], device_id_type=MESH)

    lane = lax.broadcasted_iota(jnp.int32, (8, 128), 1)
    sublane = lax.broadcasted_iota(jnp.int32, (8, 128), 0)
    first, last = lane == 0, lane == 127
    has_low = jnp.where(yz > 0, 1.0, 0.0).astype(F32)
    has_high = jnp.where(yz < 31, 1.0, 0.0).astype(F32)
    x_low = jnp.where(gx + c > 0, 1.0, 0.0).astype(F32)
    x_high = jnp.where(gx + c < 4, 1.0, 0.0).astype(F32)

    def edge_of(x):
        return jnp.where(x < 4, x_low, jnp.where(x >= 20, x_high, 1.0))

    flying = []

    def remote(src, dst, sends, recvs, device):
        return pltpu.make_async_remote_copy(
            src_ref=src, dst_ref=dst, send_sem=sends, recv_sem=recvs,
            device_id=device, device_id_type=MESH,
        )

    def send(*what):
        copy = remote(*what)
        copy.start()
        flying.append(copy)
        return copy

    def exchange(e, ref):
        out, into = ys.at[e], yr.at[e]
        plan = (
            (out.at[1], into.at[0, pl.ds(4, 16)], up),
            (out.at[0], into.at[1, pl.ds(4, 16)], down),
            (ref.at[pl.ds(4 + 12 * c, 4), :, rows], ref.at[pl.ds(20 - 20 * c, 4), :, rows], far),
            (out.at[1, pl.ds(13 * c, 3)], into.at[0, pl.ds(20 - 19 * c, 3)], far_up),
            (out.at[0, pl.ds(13 * c, 3)], into.at[1, pl.ds(20 - 19 * c, 3)], far_down),
            (out.at[1, pl.ds(13 - 13 * c, 3)], into.at[0, pl.ds(1 + 19 * c, 3)], near_up),
            (out.at[0, pl.ds(13 - 13 * c, 3)], into.at[1, pl.ds(1 + 19 * c, 3)], near_down),
            (ref.at[pl.ds(16 - 12 * c, 4), :, rows], ref.at[pl.ds(20 * c, 4), :, rows], near),
        )
        return [
            remote(src, dst, ghost_send.at[e, i], ghost_recv.at[e, i], device)
            for i, (src, dst, device) in enumerate(plan)
        ]

    def launch(e, ref):
        for copy in exchange(e, ref):
            copy.start()

    for load in loads:
        load.wait()

    def prepare(x):
        for h in range(2):
            for t in range(2):
                at = pl.ds(8 * t, 8)
                d = (damping[x, h, at] + (7.0 - MID)) * (2.0 / HALF)
                diag[x + 4, h, pl.ds(8 + 8 * t, 8)] = d
                ys[0, t, x, h] = d[4 * t : 4 * t + 4]
            ps[0, x, h] = init[x + 1, h, 8:9]
            ps[1, x, h] = init[x + 1, h, 23:24]

    planes(0, 16, 4, prepare)
    pl.semaphore_wait(barrier, 46)
    first_sends = [
        send(ps.at[1], pr.at[0], init_send.at[0], init_recv.at[0], up),
        send(ps.at[0], pr.at[1], init_send.at[1], init_recv.at[1], down),
        send(
            init.at[pl.ds(1 + 15 * c, 1), :, rows], init.at[pl.ds(17 - 17 * c, 1), :, rows],
            init_send.at[2], init_recv.at[2], far,
        ),
    ]
    launch(0, diag)

    for copy in first_sends:
        copy.wait_recv()
    for h in range(2):
        init[0, h, rows] = init[0, h, rows] * x_low
        init[17, h, rows] = init[17, h, rows] * x_high

    def neighbours_of(ref, x, at):
        v = [ref[x, h, pl.ds(at, 8)] for h in range(2)]
        n = zsum(*v, first, last)
        total = []
        for h in range(2):
            along_y = ref[x, h, pl.ds(at - 1, 8)] + ref[x, h, pl.ds(at + 1, 8)]
            total.append(n[h] + (along_y + (ref[x - 1, h, pl.ds(at, 8)] + ref[x + 1, h, pl.ds(at, 8)])))
        return v, total

    def edge_rows(x):
        for h in range(2):
            init[x + 1, h, 7:8] = pr[0, x, h] * has_low
            init[x + 1, h, 24:25] = pr[1, x, h] * has_high

    planes(0, 16, 4, edge_rows)

    def first_vector(x):
        for t in range(2):
            v, total = neighbours_of(init, x + 1, 8 + 8 * t)
            for h in range(2):
                at = pl.ds(8 * t, 8)
                w = source[x, h, at] - ((damping[x, h, at] + 6.0) * v[h] - total[h])
                vec[0, x + 4, h, pl.ds(8 + 8 * t, 8)] = w
                ys[1, t, x, h] = w[4 * t : 4 * t + 4]

    planes(0, 16, 4, first_vector)
    launch(1, vec.at[0])

    def merge(e, ref, masked):
        for copy in exchange(e, ref):
            copy.wait_recv()

        def ghosts(x):
            edge = edge_of(x) if masked else None
            for h in range(2):
                low, high = yr[e, 0, x, h], yr[e, 1, x, h]
                if masked:
                    low, high = low * (has_low * edge), high * (has_high * edge)
                ref[x, h, 4:8] = low
                ref[x, h, 24:28] = high

        planes(0, 24, 4, ghosts)
        if masked:
            for x in range(4):
                for h in range(2):
                    ref[x, h, rows] = ref[x, h, rows] * x_low
                    ref[20 + x, h, rows] = ref[20 + x, h, rows] * x_high

    merge(0, diag, False)

    def block_of(block, carry):
        base = 4 * block
        merge(block + 1, vec.at[base], True)
        for j, step in ((1, 11), (2, 5), (3, 6)):
            starts = (4 + j, 12 + j, 20 - j)
            keep = []
            for at in starts:
                r = sublane + at
                keep.append(jnp.where(r < 8, has_low, jnp.where(r >= 24, has_high, 1.0)).astype(F32))

            def apply(x, j=j, starts=starts, keep=keep):
                edge = edge_of(x)
                for at, mask in zip(starts, keep):
                    v, total = neighbours_of(vec.at[base + j - 1], x, at)
                    for h in range(2):
                        t = diag[x, h, pl.ds(at, 8)] * v[h] - total[h] * (2.0 / HALF)
                        t = 0.5 * t if j == 1 else t - vec[base + j - 2, x, h, pl.ds(at, 8)]
                        vec[base + j, x, h, pl.ds(at, 8)] = t * (mask * edge)

            planes(j, 24 - 2 * j, step, apply)

        def close(x):
            for t in range(2):
                at = 8 + 8 * t
                v, total = neighbours_of(vec.at[base + 3], x + 4, at)
                for h in range(2):
                    old = [vec[base + q, x + 4, h, pl.ds(at, 8)] for q in range(3)]
                    new = diag[x + 4, h, pl.ds(at, 8)] * v[h] - total[h] * (2.0 / HALF) - old[2]
                    new = PSI[4] * new + (PSI[3] * v[h] + PSI[2] * old[2]) + (PSI[1] * old[1] + PSI[0] * old[0])
                    vec[base + 4, x + 4, h, pl.ds(at, 8)] = new
                    ys[block + 2, t, x, h] = new[4 * t : 4 * t + 4]

        planes(0, 16, 4, close)

        @pl.when(block < 2)
        def _():
            launch(block + 2, vec.at[base + 4])

        def products(i, carry):
            for u in range(4):
                for h in range(2):
                    for t in range(2):
                        v = [vec[base + q, 4 * i + u + 4, h, pl.ds(8 + 8 * t, 8)] for q in range(5)]
                        terms = [v[0] * v[q] for q in range(4)] + [v[4] * v[q] for q in range(4)]
                        carry = tuple(a + n for a, n in zip(carry, terms))
            return carry

        totals = lax.fori_loop(0, 4, products, (jnp.zeros((8, 128), F32),) * 8)
        for q, total in enumerate(totals):
            sums[block, q : q + 1] = jnp.sum(total, axis=0, keepdims=True)
        return carry

    lax.fori_loop(0, 3, block_of, 0)

    diagonal = lax.broadcasted_iota(jnp.int32, (24, 128), 0) == lax.broadcasted_iota(jnp.int32, (24, 128), 1)

    def to_row(v):
        return jnp.sum(jnp.where(diagonal, v, 0.0), axis=0, keepdims=True)

    part_a[plane_slot] = to_row(jnp.sum(jnp.concatenate([sums[0], sums[1], sums[2]], axis=0), axis=1, keepdims=True))

    def plane_copy(k):
        slot, device = plane_mate(k)
        return slot, pltpu.make_async_remote_copy(
            src_ref=part_a.at[plane_slot], dst_ref=part_a.at[plane_slot],
            send_sem=a_send.at[slot], recv_sem=a_recv.at[plane_slot],
            device_id=device, device_id_type=MESH,
        )

    def plane_wait(k):
        slot, device = plane_mate(k)
        return pltpu.make_async_remote_copy(
            src_ref=part_a.at[slot], dst_ref=part_a.at[slot],
            send_sem=a_send.at[slot], recv_sem=a_recv.at[slot],
            device_id=device, device_id_type=MESH,
        )

    def start_plane(k, carry):
        plane_copy(k)[1].start()
        return carry

    def finish_plane(k, carry):
        plane_wait(k).wait_recv()
        return carry

    lax.fori_loop(1, 32, start_plane, 0)
    lax.fori_loop(1, 32, finish_plane, 0)
    part_b[z] = jnp.sum(part_a[...], axis=0)
    line = []
    for k in range(1, 8):
        slot, device = line_mate(k)
        copy = pltpu.make_async_remote_copy(
            src_ref=part_b.at[z], dst_ref=part_b.at[z],
            send_sem=b_send.at[slot], recv_sem=b_recv.at[z],
            device_id=device, device_id_type=MESH,
        )
        copy.start()
        line.append((slot, device))
    for slot, device in line:
        pltpu.make_async_remote_copy(
            src_ref=part_b.at[slot], dst_ref=part_b.at[slot],
            send_sem=b_send.at[slot], recv_sem=b_recv.at[slot],
            device_id=device, device_id_type=MESH,
        ).wait_recv()
    total = jnp.sum(part_b[...], axis=0)
    nu = jnp.sum(jnp.where(diagonal, total, 0.0), axis=1, keepdims=True)
    predicted, corrected = recurrences(jnp.broadcast_to(nu, (24, 128)))

    upper = jnp.where(c == 1, 1.0, 0.0).astype(F32)
    away = [corrected[k : k + 1] + upper * (predicted[k : k + 1] - corrected[k : k + 1]) for k in range(12)]
    home = [predicted[k : k + 1] + upper * (corrected[k : k + 1] - predicted[k : k + 1]) for k in range(12)]

    def combine(ref, weights):
        spread = [jnp.broadcast_to(w, (8, 128)) for w in weights]

        def body(x):
            for h in range(2):
                for t in range(2):
                    at = pl.ds(8 + 8 * t, 8)
                    terms = [spread[k] * vec[k, x + 4, h, at] for k in range(12)]
                    terms.append(init[x + 1, h, at])
                    while len(terms) > 1:
                        terms = [a + b for a, b in zip(terms[::2], terms[1::2])] + terms[len(terms) & ~1 :]
                    ref[h, x, pl.ds(8 * t, 8)] = terms[0]

        planes(0, 16, 4, body)

    def place(h, part):
        return out_hbm.at[0, pl.ds(part * 16, 16), :, pl.ds(128 * h, 128)]

    combine(theirs, away)
    for h in range(2):
        send(theirs.at[h], place(h, c), out_send.at[h], out_recv.at[h], near)
    combine(mine, home)
    keeps = [pltpu.make_async_copy(mine.at[h], place(h, c), out_sem.at[h]) for h in range(2)]
    for copy in keeps:
        copy.start()

    for copy in flying:
        copy.wait_send()
    for e, ref in enumerate((diag, vec.at[0], vec.at[4], vec.at[8])):
        for copy in exchange(e, ref):
            copy.wait_send()

    def drain(k, carry):
        plane_wait(k).wait_send()
        return carry

    lax.fori_loop(1, 32, drain, 0)
    for slot, device in line:
        pltpu.make_async_remote_copy(
            src_ref=part_b.at[z], dst_ref=part_b.at[z],
            send_sem=b_send.at[slot], recv_sem=b_recv.at[slot],
            device_id=device, device_id_type=MESH,
        ).wait_send()
    for copy in keeps:
        copy.wait()
    for h in range(2):
        remote(theirs.at[h], place(h, other), out_send.at[h], out_recv.at[h], near).wait_recv()


def per_device(init_field, source, damping):
    anywhere = pl.BlockSpec(memory_space=pl.ANY)
    dma = pltpu.SemaphoreType.DMA
    return pl.pallas_call(
        kernel,
        out_shape=jax.ShapeDtypeStruct((1, 32, 16, 256), F32),
        in_specs=[anywhere] * 3,
        out_specs=anywhere,
        scratch_shapes=[
            pltpu.VMEM((13, 24, 2, 32, 128), F32),
            pltpu.VMEM((24, 2, 32, 128), F32),
            pltpu.VMEM((18, 2, 32, 128), F32),
            pltpu.VMEM((16, 2, 16, 128), F32),
            pltpu.VMEM((16, 2, 16, 128), F32),
            pltpu.VMEM((5, 2, 16, 2, 4, 128), F32),
            pltpu.VMEM((4, 2, 24, 2, 4, 128), F32),
            pltpu.VMEM((2, 16, 2, 1, 128), F32),
            pltpu.VMEM((2, 16, 2, 1, 128), F32),
            pltpu.VMEM((3, 8, 128), F32),
            pltpu.VMEM((32, 1, 128), F32),
            pltpu.VMEM((8, 1, 128), F32),
            pltpu.VMEM((2, 16, 16, 128), F32),
            pltpu.VMEM((2, 16, 16, 128), F32),
            dma((8,)), dma((3,)), dma((3,)), dma((4, 8)), dma((4, 8)),
            dma((32,)), dma((32,)), dma((8,)), dma((8,)), dma((2,)), dma((2,)), dma((2,)),
        ],
        compiler_params=pltpu.CompilerParams(collective_id=0, has_side_effects=True),
        cost_estimate=pl.CostEstimate(flops=50_000_000, bytes_accessed=3_000_000, transcendentals=0),
    )(init_field, source, damping)


def solution(mesh):
    block = P("gx", "yz", None)
    return jax.shard_map(
        per_device,
        mesh=mesh,
        in_specs=(block, block, block),
        out_specs=P("level", "gx", "yz", None),
        check_vma=False,
    )
```

```python
import functools

import jax
import jax.numpy as jnp
import numpy as np
from jax import lax
from jax.experimental import pallas as pl
from jax.experimental.pallas import tpu as pltpu
from jax.sharding import PartitionSpec as P

STEPS = 3
ITERS = 3
MESH = pl.DeviceIdType.MESH
F32 = jnp.float32

LOW, HIGH = 1.05, 15.0
MID, HALF = (LOW + HIGH) / 2, (HIGH - LOW) / 2
W = 4
STEP_PLANES = ((1, 11), (2, 10), (3, 9))


def block_polynomial():
    cheb = np.polynomial.chebyshev
    low, high = 2.0, 13.5

    def third(lam):
        x = (lam - (low + high) / 2) / ((high - low) / 2)
        return 4 * x**3 - 3 * x

    nodes = np.cos(np.pi * (np.arange(4) + 0.5) / 4)
    lam = MID + HALF * nodes
    rho = cheb.chebfit(nodes, (1 + (lam - 1) * third(lam) / third(0.0)) / lam, 3)
    return [float(c) for c in cheb.chebmul(rho, [0.0, 1.0])]


PSI = block_polynomial()


def planes(start, count, step, body):
    def turn(i, carry):
        for u in range(step):
            body(start + i * step + u)
        return carry

    lax.fori_loop(0, count // step, turn, 0)


def zsum(v0, v1, first, last):
    a0, a1 = pltpu.roll(v0, 1, 1), pltpu.roll(v1, 1, 1)
    b0, b1 = pltpu.roll(v0, 127, 1), pltpu.roll(v1, 127, 1)
    n0 = jnp.where(first, 0.0, a0) + jnp.where(last, b1, b0)
    n1 = jnp.where(first, a0, a1) + jnp.where(last, 0.0, b1)
    return n0, n1


def recurrences(nu):
    c0, c1, c2, c3, c4 = PSI

    def pattern(rows, values):
        j = lax.rem(lax.broadcasted_iota(jnp.int32, (rows, 128), 0), 4)
        out = jnp.full((rows, 128), values[3], F32)
        for q in range(3):
            out = jnp.where(j == q, values[q], out)
        return out

    bands = {
        1: (1.0, 0.5, 0.5, 0.5 / c4),
        -1: (0.0, 0.5, 0.5, 0.5 - 0.5 * c2 / c4),
        0: (0.0, 0.0, 0.0, -0.5 * c3 / c4),
        -2: (0.0, 0.0, 0.0, -0.5 * c1 / c4),
        -3: (0.0, 0.0, 0.0, -0.5 * c0 / c4),
    }
    long = {o: pattern(24, v) for o, v in bands.items()}
    short = {o: pattern(16, v) for o, v in bands.items()}

    def shifted(v, o):
        rows = v.shape[0]
        return v if o % rows == 0 else pltpu.roll(v, o % rows, 0)

    def times(z, shift):
        f, m = z
        fx = sum(shifted(f * short[o], o) for o in bands)
        mx = sum(long[o] * shifted(m, -o) for o in bands)
        return fx + shift * f, mx + shift * m

    def inner(y, z):
        return jnp.sum(y[0] * z[1][:16], axis=0, keepdims=True)

    def axpy(y, s, z):
        return y[0] + s * z[0], y[1] + s * z[1]

    one = jnp.where(lax.broadcasted_iota(jnp.int32, (16, 128), 0) == 0, 1.0, 0.0).astype(F32)
    start = (one, nu)

    def solve(resid, answer):
        direction = resid
        norm = inner(resid, resid)
        for step in range(ITERS):
            image = times(direction, MID / HALF)
            alpha = norm / inner(direction, image)
            answer = axpy(answer, alpha, direction) if answer else (alpha * direction[0], alpha * direction[1])
            if step + 1 < ITERS:
                resid = axpy(resid, -alpha, image)
                following = inner(resid, resid)
                direction = axpy(resid, following / norm, direction)
                norm = following
        return answer

    back = (MID - 1.0) / HALF
    states = [None]
    corrected = None
    for step in range(STEPS):
        state = states[-1]
        resid = axpy(start, -1.0, times(state, back)) if state else start
        states.append(solve(resid, state))
        change = axpy(states[-1], -1.0, state) if state else states[-1]
        inside = axpy(corrected, -0.5, change) if corrected else (-0.5 * change[0], -0.5 * change[1])
        resid = axpy(start, -1.0, times(inside, back))
        corrected = solve(resid, corrected)
    return states[-1][0] * (1.0 / HALF), corrected[0] * (1.0 / HALF)


def kernel(
    init_hbm, source_hbm, damping_hbm, out_hbm,
    u0, u1, u2, u3, diag, init, source, damping, ys, yr, ps, pr, sums, part_a, part_b, mine, theirs,
    local_sem, init_send, init_recv, ghost_send, ghost_recv,
    a_send, a_recv, b_send, b_recv, out_sem, out_send, out_recv,
):
    c = lax.axis_index("level")
    gx = lax.axis_index("gx")
    yz = lax.axis_index("yz")
    other = 1 - c
    beyond = lax.rem(gx + 2 * c + 3, 4)
    above, below = lax.rem(yz + 1, 32), lax.rem(yz + 31, 32)
    far, near = (other, beyond, yz), (other, gx, yz)
    up, down = (c, gx, above), (c, gx, below)
    far_up, far_down = (other, beyond, above), (other, beyond, below)
    near_up, near_down = (other, gx, above), (other, gx, below)
    neighbours = (far, near, up, down, far_up, far_down, near_up, near_down)
    y, z = lax.rem(yz, 4), lax.div(yz, 4)
    plane_slot = gx * 8 + c * 4 + y

    def plane_mate(k):
        slot = lax.rem(plane_slot + k, 32)
        return slot, (lax.rem(lax.div(slot, 4), 2), lax.div(slot, 8), z * 4 + lax.rem(slot, 4))

    def line_mate(k):
        slot = lax.rem(z + k, 8)
        return slot, (c, gx, slot * 4 + y)

    own = pl.ds(c * 16, 16)
    rows = pl.ds(8, 16)
    loads = []
    for h in range(2):
        s = pl.ds(128 * h, 128)
        loads += [
            pltpu.make_async_copy(damping_hbm.at[own, :, s], damping.at[:, h], local_sem.at[h]),
            pltpu.make_async_copy(init_hbm.at[own, :, s], init.at[pl.ds(1, 16), h, rows], local_sem.at[2 + h]),
            pltpu.make_async_copy(
                init_hbm.at[pl.ds(16 - c, 1), :, s], init.at[pl.ds(17 - 17 * c, 1), h, rows], local_sem.at[4 + h]
            ),
            pltpu.make_async_copy(source_hbm.at[own, :, s], source.at[:, h], local_sem.at[6 + h]),
        ]
    for load in loads:
        load.start()

    barrier = pltpu.get_barrier_semaphore()
    for k in range(1, 8):
        pl.semaphore_signal(barrier, inc=1, device_id=line_mate(k)[1], device_id_type=MESH)
    for device in neighbours:
        pl.semaphore_signal(barrier, inc=1, device_id=device, device_id_type=MESH)
    for k in range(1, 32):
        pl.semaphore_signal(barrier, inc=1, device_id=plane_mate(k)[1], device_id_type=MESH)

    lane = lax.broadcasted_iota(jnp.int32, (8, 128), 1)
    sublane = lax.broadcasted_iota(jnp.int32, (8, 128), 0)
    first, last = lane == 0, lane == 127
    has_low = jnp.where(yz > 0, 1.0, 0.0).astype(F32)
    has_high = jnp.where(yz < 31, 1.0, 0.0).astype(F32)
    x_low = jnp.where(gx + c > 0, 1.0, 0.0).astype(F32)
    x_high = jnp.where(gx + c < 4, 1.0, 0.0).astype(F32)

    def edge_of(x):
        return jnp.where(x < 4, x_low, jnp.where(x >= 20, x_high, 1.0))

    flying = []

    def remote(src, dst, sends, recvs, device):
        return pltpu.make_async_remote_copy(
            src_ref=src, dst_ref=dst, send_sem=sends, recv_sem=recvs,
            device_id=device, device_id_type=MESH,
        )

    def send(*what):
        copy = remote(*what)
        copy.start()
        flying.append(copy)
        return copy

    def exchange(e, ref):
        out, into = ys.at[e], yr.at[e]
        plan = (
            (out.at[1], into.at[0, pl.ds(4, 16)], up),
            (out.at[0], into.at[1, pl.ds(4, 16)], down),
            (ref.at[pl.ds(4 + 12 * c, 4), :, rows], ref.at[pl.ds(20 - 20 * c, 4), :, rows], far),
            (out.at[1, pl.ds(13 * c, 3)], into.at[0, pl.ds(20 - 19 * c, 3)], far_up),
            (out.at[0, pl.ds(13 * c, 3)], into.at[1, pl.ds(20 - 19 * c, 3)], far_down),
            (out.at[1, pl.ds(13 - 13 * c, 3)], into.at[0, pl.ds(1 + 19 * c, 3)], near_up),
            (out.at[0, pl.ds(13 - 13 * c, 3)], into.at[1, pl.ds(1 + 19 * c, 3)], near_down),
            (ref.at[pl.ds(16 - 12 * c, 4), :, rows], ref.at[pl.ds(20 * c, 4), :, rows], near),
        )
        return [
            remote(src, dst, ghost_send.at[e, i], ghost_recv.at[e, i], device)
            for i, (src, dst, device) in enumerate(plan)
        ]

    def launch(e, ref):
        for copy in exchange(e, ref):
            copy.start()

    for load in loads:
        load.wait()

    def prepare(x):
        for h in range(2):
            for t in range(2):
                at = pl.ds(8 * t, 8)
                d = (damping[x, h, at] + (7.0 - MID)) * (2.0 / HALF)
                diag[x + 4, h, pl.ds(8 + 8 * t, 8)] = d
                ys[0, t, x, h] = d[4 * t : 4 * t + 4]
            ps[0, x, h] = init[x + 1, h, 8:9]
            ps[1, x, h] = init[x + 1, h, 23:24]

    planes(0, 16, 4, prepare)
    pl.semaphore_wait(barrier, 46)
    first_sends = [
        send(ps.at[1], pr.at[0], init_send.at[0], init_recv.at[0], up),
        send(ps.at[0], pr.at[1], init_send.at[1], init_recv.at[1], down),
        send(
            init.at[pl.ds(1 + 15 * c, 1), :, rows], init.at[pl.ds(17 - 17 * c, 1), :, rows],
            init_send.at[2], init_recv.at[2], far,
        ),
    ]
    launch(0, diag)

    for copy in first_sends:
        copy.wait_recv()
    for h in range(2):
        init[0, h, rows] = init[0, h, rows] * x_low
        init[17, h, rows] = init[17, h, rows] * x_high

    def neighbours_of(ref, x, at):
        v = [ref[x, h, pl.ds(at, 8)] for h in range(2)]
        n = zsum(*v, first, last)
        total = []
        for h in range(2):
            along_y = ref[x, h, pl.ds(at - 1, 8)] + ref[x, h, pl.ds(at + 1, 8)]
            total.append(n[h] + (along_y + (ref[x - 1, h, pl.ds(at, 8)] + ref[x + 1, h, pl.ds(at, 8)])))
        return v, total

    def edge_rows(x):
        for h in range(2):
            init[x + 1, h, 7:8] = pr[0, x, h] * has_low
            init[x + 1, h, 24:25] = pr[1, x, h] * has_high

    planes(0, 16, 4, edge_rows)

    def first_vector(x):
        for t in range(2):
            v, total = neighbours_of(init, x + 1, 8 + 8 * t)
            for h in range(2):
                at = pl.ds(8 * t, 8)
                w = source[x, h, at] - ((damping[x, h, at] + 6.0) * v[h] - total[h])
                u0[0, x + 4, h, pl.ds(8 + 8 * t, 8)] = w
                ys[1, t, x, h] = w[4 * t : 4 * t + 4]

    planes(0, 16, 4, first_vector)
    launch(1, u0.at[0])

    def merge(e, ref, masked):
        for copy in exchange(e, ref):
            copy.wait_recv()

        def ghosts(x):
            edge = edge_of(x) if masked else None
            for h in range(2):
                low, high = yr[e, 0, x, h], yr[e, 1, x, h]
                if masked:
                    low, high = low * (has_low * edge), high * (has_high * edge)
                ref[x, h, 4:8] = low
                ref[x, h, 24:28] = high

        planes(0, 24, 4, ghosts)
        if masked:
            for x in range(4):
                for h in range(2):
                    ref[x, h, rows] = ref[x, h, rows] * x_low
                    ref[20 + x, h, rows] = ref[20 + x, h, rows] * x_high

    merge(0, diag, False)

    def block_of(block, carry):
        basis = [u.at[block] for u in (u0, u1, u2, u3)]
        following = u0.at[block + 1]
        merge(block + 1, basis[0], True)
        for j, step in STEP_PLANES:
            starts = (4 + j, 12 + j, 20 - j)
            keep = []
            for at in starts:
                r = sublane + at
                keep.append(jnp.where(r < 8, has_low, jnp.where(r >= 24, has_high, 1.0)).astype(F32))

            def apply(x, j=j, starts=starts, keep=keep):
                edge = edge_of(x)
                for at, mask in zip(starts, keep):
                    v, total = neighbours_of(basis[j - 1], x, at)
                    for h in range(2):
                        t = diag[x, h, pl.ds(at, 8)] * v[h] - total[h] * (2.0 / HALF)
                        t = 0.5 * t if j == 1 else t - basis[j - 2][x, h, pl.ds(at, 8)]
                        basis[j][x, h, pl.ds(at, 8)] = t * (mask * edge)

            planes(j, 24 - 2 * j, step, apply)

        def close(i, carry):
            done = []
            for u in range(8):
                x = 8 * i + u + 4
                for at in (8, 16):
                    v, total = neighbours_of(basis[3], x, at)
                    for h in range(2):
                        old = [basis[q][x, h, pl.ds(at, 8)] for q in range(3)]
                        new = diag[x, h, pl.ds(at, 8)] * v[h] - total[h] * (2.0 / HALF) - old[2]
                        new = PSI[4] * new + (PSI[3] * v[h] + PSI[2] * old[2]) + (PSI[1] * old[1] + PSI[0] * old[0])
                        done.append((x, h, at, new))
            for x, h, at, new in done:
                following[x, h, pl.ds(at, 8)] = new
                t = at // 8 - 1
                ys[block + 2, t, x - 4, h] = new[4 * t : 4 * t + 4]
            return carry

        lax.fori_loop(0, 2, close, 0)

        @pl.when(block < 2)
        def _():
            launch(block + 2, following)

        def products(i, carry):
            for u in range(4):
                for h in range(2):
                    for t in range(2):
                        v = [f[4 * i + u + 4, h, pl.ds(8 + 8 * t, 8)] for f in (*basis, following)]
                        terms = [v[0] * v[q] for q in range(4)] + [v[4] * v[q] for q in range(4)]
                        carry = tuple(a + n for a, n in zip(carry, terms))
            return carry

        totals = lax.fori_loop(0, 4, products, (jnp.zeros((8, 128), F32),) * 8)
        for q, total in enumerate(totals):
            sums[block, q : q + 1] = jnp.sum(total, axis=0, keepdims=True)
        return carry

    lax.fori_loop(0, 3, block_of, 0)

    diagonal = lax.broadcasted_iota(jnp.int32, (24, 128), 0) == lax.broadcasted_iota(jnp.int32, (24, 128), 1)

    def to_row(v):
        return jnp.sum(jnp.where(diagonal, v, 0.0), axis=0, keepdims=True)

    part_a[plane_slot] = to_row(jnp.sum(jnp.concatenate([sums[0], sums[1], sums[2]], axis=0), axis=1, keepdims=True))

    def plane_copy(k):
        slot, device = plane_mate(k)
        return slot, pltpu.make_async_remote_copy(
            src_ref=part_a.at[plane_slot], dst_ref=part_a.at[plane_slot],
            send_sem=a_send.at[slot], recv_sem=a_recv.at[plane_slot],
            device_id=device, device_id_type=MESH,
        )

    def plane_wait(k):
        slot, device = plane_mate(k)
        return pltpu.make_async_remote_copy(
            src_ref=part_a.at[slot], dst_ref=part_a.at[slot],
            send_sem=a_send.at[slot], recv_sem=a_recv.at[slot],
            device_id=device, device_id_type=MESH,
        )

    def start_plane(k, carry):
        plane_copy(k)[1].start()
        return carry

    def finish_plane(k, carry):
        plane_wait(k).wait_recv()
        return carry

    lax.fori_loop(1, 32, start_plane, 0)
    lax.fori_loop(1, 32, finish_plane, 0)
    part_b[z] = jnp.sum(part_a[...], axis=0)
    line = []
    for k in range(1, 8):
        slot, device = line_mate(k)
        copy = pltpu.make_async_remote_copy(
            src_ref=part_b.at[z], dst_ref=part_b.at[z],
            send_sem=b_send.at[slot], recv_sem=b_recv.at[z],
            device_id=device, device_id_type=MESH,
        )
        copy.start()
        line.append((slot, device))
    for slot, device in line:
        pltpu.make_async_remote_copy(
            src_ref=part_b.at[slot], dst_ref=part_b.at[slot],
            send_sem=b_send.at[slot], recv_sem=b_recv.at[slot],
            device_id=device, device_id_type=MESH,
        ).wait_recv()
    total = jnp.sum(part_b[...], axis=0)
    nu = jnp.sum(jnp.where(diagonal, total, 0.0), axis=1, keepdims=True)
    predicted, corrected = recurrences(jnp.broadcast_to(nu, (24, 128)))

    upper = jnp.where(c == 1, 1.0, 0.0).astype(F32)
    away = [corrected[k : k + 1] + upper * (predicted[k : k + 1] - corrected[k : k + 1]) for k in range(12)]
    home = [predicted[k : k + 1] + upper * (corrected[k : k + 1] - predicted[k : k + 1]) for k in range(12)]

    def combine(ref, weights):
        spread = [jnp.broadcast_to(w, (8, 128)) for w in weights]

        def body(x):
            for h in range(2):
                for t in range(2):
                    at = pl.ds(8 + 8 * t, 8)
                    terms = [spread[k] * (u0, u1, u2, u3)[k % 4][k // 4, x + 4, h, at] for k in range(12)]
                    terms.append(init[x + 1, h, at])
                    while len(terms) > 1:
                        terms = [a + b for a, b in zip(terms[::2], terms[1::2])] + terms[len(terms) & ~1 :]
                    ref[h, x, pl.ds(8 * t, 8)] = terms[0]

        planes(0, 16, 4, body)

    def place(h, part):
        return out_hbm.at[0, pl.ds(part * 16, 16), :, pl.ds(128 * h, 128)]

    combine(theirs, away)
    for h in range(2):
        send(theirs.at[h], place(h, c), out_send.at[h], out_recv.at[h], near)
    combine(mine, home)
    keeps = [pltpu.make_async_copy(mine.at[h], place(h, c), out_sem.at[h]) for h in range(2)]
    for copy in keeps:
        copy.start()

    for copy in flying:
        copy.wait_send()
    for e, ref in enumerate((diag, u0.at[0], u0.at[1], u0.at[2])):
        for copy in exchange(e, ref):
            copy.wait_send()

    def drain(k, carry):
        plane_wait(k).wait_send()
        return carry

    lax.fori_loop(1, 32, drain, 0)
    for slot, device in line:
        pltpu.make_async_remote_copy(
            src_ref=part_b.at[z], dst_ref=part_b.at[z],
            send_sem=b_send.at[slot], recv_sem=b_recv.at[slot],
            device_id=device, device_id_type=MESH,
        ).wait_send()
    for copy in keeps:
        copy.wait()
    for h in range(2):
        remote(theirs.at[h], place(h, other), out_send.at[h], out_recv.at[h], near).wait_recv()


def per_device(init_field, source, damping):
    anywhere = pl.BlockSpec(memory_space=pl.ANY)
    dma = pltpu.SemaphoreType.DMA
    return pl.pallas_call(
        kernel,
        out_shape=jax.ShapeDtypeStruct((1, 32, 16, 256), F32),
        in_specs=[anywhere] * 3,
        out_specs=anywhere,
        scratch_shapes=[
            pltpu.VMEM((4, 24, 2, 32, 128), F32),
            pltpu.VMEM((3, 24, 2, 32, 128), F32),
            pltpu.VMEM((3, 24, 2, 32, 128), F32),
            pltpu.VMEM((3, 24, 2, 32, 128), F32),
            pltpu.VMEM((24, 2, 32, 128), F32),
            pltpu.VMEM((18, 2, 32, 128), F32),
            pltpu.VMEM((16, 2, 16, 128), F32),
            pltpu.VMEM((16, 2, 16, 128), F32),
            pltpu.VMEM((5, 2, 16, 2, 4, 128), F32),
            pltpu.VMEM((4, 2, 24, 2, 4, 128), F32),
            pltpu.VMEM((2, 16, 2, 1, 128), F32),
            pltpu.VMEM((2, 16, 2, 1, 128), F32),
            pltpu.VMEM((3, 8, 128), F32),
            pltpu.VMEM((32, 1, 128), F32),
            pltpu.VMEM((8, 1, 128), F32),
            pltpu.VMEM((2, 16, 16, 128), F32),
            pltpu.VMEM((2, 16, 16, 128), F32),
            dma((8,)), dma((3,)), dma((3,)), dma((4, 8)), dma((4, 8)),
            dma((32,)), dma((32,)), dma((8,)), dma((8,)), dma((2,)), dma((2,)), dma((2,)),
        ],
        compiler_params=pltpu.CompilerParams(collective_id=0, has_side_effects=True),
        cost_estimate=pl.CostEstimate(flops=50_000_000, bytes_accessed=3_000_000, transcendentals=0),
    )(init_field, source, damping)


def solution(mesh):
    block = P("gx", "yz", None)
    return jax.shard_map(
        per_device,
        mesh=mesh,
        in_specs=(block, block, block),
        out_specs=P("level", "gx", "yz", None),
        check_vma=False,
    )
```

```python
import functools

import jax
import jax.numpy as jnp
import numpy as np
from jax import lax
from jax.experimental import pallas as pl
from jax.experimental.pallas import tpu as pltpu
from jax.sharding import PartitionSpec as P

STEPS = 3
ITERS = 3
MESH = pl.DeviceIdType.MESH
F32 = jnp.float32

LOW, HIGH = 1.05, 15.0
MID, HALF = (LOW + HIGH) / 2, (HIGH - LOW) / 2
W = 4
STEP_PLANES = ((1, 11), (2, 10), (3, 9))


def block_polynomial():
    cheb = np.polynomial.chebyshev
    low, high = 2.0, 13.5

    def third(lam):
        x = (lam - (low + high) / 2) / ((high - low) / 2)
        return 4 * x**3 - 3 * x

    nodes = np.cos(np.pi * (np.arange(4) + 0.5) / 4)
    lam = MID + HALF * nodes
    rho = cheb.chebfit(nodes, (1 + (lam - 1) * third(lam) / third(0.0)) / lam, 3)
    return [float(c) for c in cheb.chebmul(rho, [0.0, 1.0])]


PSI = block_polynomial()


def planes(start, count, step, body):
    def turn(i, carry):
        for u in range(step):
            body(start + i * step + u)
        return carry

    lax.fori_loop(0, count // step, turn, 0)


def zsum(v0, v1, first, last):
    a0, a1 = pltpu.roll(v0, 1, 1), pltpu.roll(v1, 1, 1)
    b0, b1 = pltpu.roll(v0, 127, 1), pltpu.roll(v1, 127, 1)
    n0 = jnp.where(first, 0.0, a0) + jnp.where(last, b1, b0)
    n1 = jnp.where(first, a0, a1) + jnp.where(last, 0.0, b1)
    return n0, n1


def recurrences(nu):
    c0, c1, c2, c3, c4 = PSI

    def pattern(rows, values):
        j = lax.rem(lax.broadcasted_iota(jnp.int32, (rows, 128), 0), 4)
        out = jnp.full((rows, 128), values[3], F32)
        for q in range(3):
            out = jnp.where(j == q, values[q], out)
        return out

    bands = {
        1: (1.0, 0.5, 0.5, 0.5 / c4),
        -1: (0.0, 0.5, 0.5, 0.5 - 0.5 * c2 / c4),
        0: (0.0, 0.0, 0.0, -0.5 * c3 / c4),
        -2: (0.0, 0.0, 0.0, -0.5 * c1 / c4),
        -3: (0.0, 0.0, 0.0, -0.5 * c0 / c4),
    }
    long = {o: pattern(24, v) for o, v in bands.items()}
    short = {o: pattern(16, v) for o, v in bands.items()}

    def shifted(v, o):
        rows = v.shape[0]
        return v if o % rows == 0 else pltpu.roll(v, o % rows, 0)

    def times(z, shift):
        f, m = z
        fx = sum(shifted(f * short[o], o) for o in bands)
        mx = sum(long[o] * shifted(m, -o) for o in bands)
        return fx + shift * f, mx + shift * m

    def inner(y, z):
        return jnp.sum(y[0] * z[1][:16], axis=0, keepdims=True)

    def axpy(y, s, z):
        return y[0] + s * z[0], y[1] + s * z[1]

    one = jnp.where(lax.broadcasted_iota(jnp.int32, (16, 128), 0) == 0, 1.0, 0.0).astype(F32)
    start = (one, nu)

    def solve(resid, answer):
        direction = resid
        norm = inner(resid, resid)
        for step in range(ITERS):
            image = times(direction, MID / HALF)
            alpha = norm / inner(direction, image)
            answer = axpy(answer, alpha, direction) if answer else (alpha * direction[0], alpha * direction[1])
            if step + 1 < ITERS:
                resid = axpy(resid, -alpha, image)
                following = inner(resid, resid)
                direction = axpy(resid, following / norm, direction)
                norm = following
        return answer

    back = (MID - 1.0) / HALF
    states = [None]
    corrected = None
    for step in range(STEPS):
        state = states[-1]
        resid = axpy(start, -1.0, times(state, back)) if state else start
        states.append(solve(resid, state))
        change = axpy(states[-1], -1.0, state) if state else states[-1]
        inside = axpy(corrected, -0.5, change) if corrected else (-0.5 * change[0], -0.5 * change[1])
        resid = axpy(start, -1.0, times(inside, back))
        corrected = solve(resid, corrected)
    return states[-1][0] * (1.0 / HALF), corrected[0] * (1.0 / HALF)


def kernel(
    init_hbm, source_hbm, damping_hbm, out_hbm,
    u0, u1, u2, u3, diag, init, source, damping, ys, yr, ps, pr, sums, part_a, part_b, mine, theirs,
    local_sem, init_send, init_recv, ghost_send, ghost_recv,
    a_send, a_recv, b_send, b_recv, out_sem, out_send, out_recv,
):
    c = lax.axis_index("level")
    gx = lax.axis_index("gx")
    yz = lax.axis_index("yz")
    other = 1 - c
    beyond = lax.rem(gx + 2 * c + 3, 4)
    above, below = lax.rem(yz + 1, 32), lax.rem(yz + 31, 32)
    device_of = {
        "near": (other, gx, yz), "up": (c, gx, above), "down": (c, gx, below), "far": (other, beyond, yz),
        "near_up": (other, gx, above), "near_down": (other, gx, below),
        "far_up": (other, beyond, above), "far_down": (other, beyond, below),
    }
    y, z = lax.rem(yz, 4), lax.div(yz, 4)
    plane_slot = gx * 8 + c * 4 + y

    def plane_mate(k):
        slot = lax.rem(plane_slot + k, 32)
        return slot, (lax.rem(lax.div(slot, 4), 2), lax.div(slot, 8), z * 4 + lax.rem(slot, 4))

    def line_mate(k):
        slot = lax.rem(z + k, 8)
        return slot, (c, gx, slot * 4 + y)

    low_ok, high_ok = yz > 0, yz < 31
    x_low_ok, x_high_ok = gx + c > 0, gx + c < 4
    far_ok = jnp.logical_and(gx + 2 * c >= 1, gx + 2 * c <= 4)
    exists = {
        "near": None, "up": high_ok, "down": low_ok, "far": far_ok, "near_up": high_ok, "near_down": low_ok,
        "far_up": jnp.logical_and(far_ok, high_ok), "far_down": jnp.logical_and(far_ok, low_ok),
    }

    def where_there(name, act):
        if exists[name] is None:
            act()
        else:
            pl.when(exists[name])(act)
    own = pl.ds(c * 16, 16)
    rows = pl.ds(8, 16)
    loads = []
    for h in range(2):
        s = pl.ds(128 * h, 128)
        loads += [
            pltpu.make_async_copy(damping_hbm.at[own, :, s], damping.at[:, h], local_sem.at[h]),
            pltpu.make_async_copy(init_hbm.at[own, :, s], init.at[pl.ds(1, 16), h, rows], local_sem.at[2 + h]),
            pltpu.make_async_copy(
                init_hbm.at[pl.ds(16 - c, 1), :, s], init.at[pl.ds(17 - 17 * c, 1), h, rows], local_sem.at[4 + h]
            ),
            pltpu.make_async_copy(source_hbm.at[own, :, s], source.at[:, h], local_sem.at[6 + h]),
        ]
    for load in loads:
        load.start()

    barrier = pltpu.get_barrier_semaphore()
    for k in range(1, 8):
        pl.semaphore_signal(barrier, inc=1, device_id=line_mate(k)[1], device_id_type=MESH)
    greeted = 38
    for name, there in exists.items():
        where_there(
            name,
            lambda name=name: pl.semaphore_signal(barrier, inc=1, device_id=device_of[name], device_id_type=MESH),
        )
        greeted = greeted + (1 if there is None else there.astype(jnp.int32))
    for k in range(1, 32):
        pl.semaphore_signal(barrier, inc=1, device_id=plane_mate(k)[1], device_id_type=MESH)

    lane = lax.broadcasted_iota(jnp.int32, (8, 128), 1)
    sublane = lax.broadcasted_iota(jnp.int32, (8, 128), 0)
    first, last = lane == 0, lane == 127
    has_low, has_high = low_ok.astype(F32), high_ok.astype(F32)
    x_low, x_high = x_low_ok.astype(F32), x_high_ok.astype(F32)

    def edge_of(x):
        return jnp.where(x < 4, x_low, jnp.where(x >= 20, x_high, 1.0))

    def remote(src, dst, sends, recvs, name):
        return pltpu.make_async_remote_copy(
            src_ref=src, dst_ref=dst, send_sem=sends, recv_sem=recvs,
            device_id=device_of[name], device_id_type=MESH,
        )

    def exchange(e, ref):
        out, into = ys.at[e], yr.at[e]
        plan = (
            (out.at[1], into.at[0, pl.ds(4, 16)], "up"),
            (out.at[0], into.at[1, pl.ds(4, 16)], "down"),
            (ref.at[pl.ds(4 + 12 * c, 4), :, rows], ref.at[pl.ds(20 - 20 * c, 4), :, rows], "far"),
            (out.at[1, pl.ds(13 * c, 3)], into.at[0, pl.ds(20 - 19 * c, 3)], "far_up"),
            (out.at[0, pl.ds(13 * c, 3)], into.at[1, pl.ds(20 - 19 * c, 3)], "far_down"),
            (out.at[1, pl.ds(13 - 13 * c, 3)], into.at[0, pl.ds(1 + 19 * c, 3)], "near_up"),
            (out.at[0, pl.ds(13 - 13 * c, 3)], into.at[1, pl.ds(1 + 19 * c, 3)], "near_down"),
            (ref.at[pl.ds(16 - 12 * c, 4), :, rows], ref.at[pl.ds(20 * c, 4), :, rows], "near"),
        )
        return [
            (name, remote(src, dst, ghost_send.at[e, i], ghost_recv.at[e, i], name))
            for i, (src, dst, name) in enumerate(plan)
        ]

    def launch(copies):
        for name, copy in copies:
            where_there(name, copy.start)

    def receive(copies):
        for name, copy in copies:
            turned = name.replace("up", "down") if "up" in name else name.replace("down", "up")
            where_there(turned, copy.wait_recv)

    def sent(copies):
        for name, copy in copies:
            where_there(name, copy.wait_send)

    for load in loads:
        load.wait()

    def prepare(x):
        for h in range(2):
            for t in range(2):
                at = pl.ds(8 * t, 8)
                d = (damping[x, h, at] + (7.0 - MID)) * (2.0 / HALF)
                diag[x + 4, h, pl.ds(8 + 8 * t, 8)] = d
                ys[0, t, x, h] = d[4 * t : 4 * t + 4]
            ps[0, x, h] = init[x + 1, h, 8:9]
            ps[1, x, h] = init[x + 1, h, 23:24]

    planes(0, 16, 4, prepare)
    pl.semaphore_wait(barrier, greeted)
    edges = [
        ("up", remote(ps.at[1], pr.at[0], init_send.at[0], init_recv.at[0], "up")),
        ("down", remote(ps.at[0], pr.at[1], init_send.at[1], init_recv.at[1], "down")),
        ("far", remote(
            init.at[pl.ds(1 + 15 * c, 1), :, rows], init.at[pl.ds(17 - 17 * c, 1), :, rows],
            init_send.at[2], init_recv.at[2], "far",
        )),
    ]
    launch(edges)
    launch(exchange(0, diag))
    receive(edges)
    for h in range(2):
        init[0, h, rows] = jnp.where(x_low_ok, init[0, h, rows], 0.0)
        init[17, h, rows] = jnp.where(x_high_ok, init[17, h, rows], 0.0)

    def neighbours_of(ref, x, at):
        v = [ref[x, h, pl.ds(at, 8)] for h in range(2)]
        n = zsum(*v, first, last)
        total = []
        for h in range(2):
            along_y = ref[x, h, pl.ds(at - 1, 8)] + ref[x, h, pl.ds(at + 1, 8)]
            total.append(n[h] + (along_y + (ref[x - 1, h, pl.ds(at, 8)] + ref[x + 1, h, pl.ds(at, 8)])))
        return v, total

    def edge_rows(x):
        for h in range(2):
            init[x + 1, h, 7:8] = jnp.where(low_ok, pr[0, x, h], 0.0)
            init[x + 1, h, 24:25] = jnp.where(high_ok, pr[1, x, h], 0.0)

    planes(0, 16, 4, edge_rows)

    def first_vector(x):
        for t in range(2):
            v, total = neighbours_of(init, x + 1, 8 + 8 * t)
            for h in range(2):
                at = pl.ds(8 * t, 8)
                w = source[x, h, at] - ((damping[x, h, at] + 6.0) * v[h] - total[h])
                u0[0, x + 4, h, pl.ds(8 + 8 * t, 8)] = w
                ys[1, t, x, h] = w[4 * t : 4 * t + 4]

    planes(0, 16, 4, first_vector)
    launch(exchange(1, u0.at[0]))

    def merge(e, ref):
        receive(exchange(e, ref))

        def ghosts(x):
            x_in = jnp.logical_and(jnp.logical_or(x >= 4, x_low_ok), jnp.logical_or(x < 20, x_high_ok))
            low_in, high_in = jnp.logical_and(low_ok, x_in), jnp.logical_and(high_ok, x_in)
            for h in range(2):
                ref[x, h, 4:8] = jnp.where(low_in, yr[e, 0, x, h], 0.0)
                ref[x, h, 24:28] = jnp.where(high_in, yr[e, 1, x, h], 0.0)

        planes(0, 24, 4, ghosts)
        for x in range(4):
            for h in range(2):
                ref[x, h, rows] = jnp.where(x_low_ok, ref[x, h, rows], 0.0)
                ref[20 + x, h, rows] = jnp.where(x_high_ok, ref[20 + x, h, rows], 0.0)

    merge(0, diag)

    def block_of(block, carry):
        basis = [u.at[block] for u in (u0, u1, u2, u3)]
        following = u0.at[block + 1]
        merge(block + 1, basis[0])
        for j, step in STEP_PLANES:
            starts = (4 + j, 12 + j, 20 - j)
            keep = []
            for at in starts:
                r = sublane + at
                keep.append(jnp.where(r < 8, has_low, jnp.where(r >= 24, has_high, 1.0)).astype(F32))

            def apply(x, j=j, starts=starts, keep=keep):
                edge = edge_of(x)
                for at, mask in zip(starts, keep):
                    v, total = neighbours_of(basis[j - 1], x, at)
                    for h in range(2):
                        t = diag[x, h, pl.ds(at, 8)] * v[h] - total[h] * (2.0 / HALF)
                        t = 0.5 * t if j == 1 else t - basis[j - 2][x, h, pl.ds(at, 8)]
                        basis[j][x, h, pl.ds(at, 8)] = t * (mask * edge)

            planes(j, 24 - 2 * j, step, apply)

        def close(i, carry):
            done = []
            for u in range(8):
                x = 8 * i + u + 4
                for at in (8, 16):
                    v, total = neighbours_of(basis[3], x, at)
                    for h in range(2):
                        old = [basis[q][x, h, pl.ds(at, 8)] for q in range(3)]
                        new = diag[x, h, pl.ds(at, 8)] * v[h] - total[h] * (2.0 / HALF) - old[2]
                        new = PSI[4] * new + (PSI[3] * v[h] + PSI[2] * old[2]) + (PSI[1] * old[1] + PSI[0] * old[0])
                        done.append((x, h, at, new))
            for x, h, at, new in done:
                following[x, h, pl.ds(at, 8)] = new
                t = at // 8 - 1
                ys[block + 2, t, x - 4, h] = new[4 * t : 4 * t + 4]
            return carry

        lax.fori_loop(0, 2, close, 0)

        @pl.when(block < 2)
        def _():
            launch(exchange(block + 2, following))

        def products(i, carry):
            for u in range(4):
                for h in range(2):
                    for t in range(2):
                        v = [f[4 * i + u + 4, h, pl.ds(8 + 8 * t, 8)] for f in (*basis, following)]
                        terms = [v[0] * v[q] for q in range(4)] + [v[4] * v[q] for q in range(4)]
                        carry = tuple(a + n for a, n in zip(carry, terms))
            return carry

        totals = lax.fori_loop(0, 4, products, (jnp.zeros((8, 128), F32),) * 8)
        for q, total in enumerate(totals):
            sums[block, q : q + 1] = jnp.sum(total, axis=0, keepdims=True)
        return carry

    lax.fori_loop(0, 3, block_of, 0)

    diagonal = lax.broadcasted_iota(jnp.int32, (24, 128), 0) == lax.broadcasted_iota(jnp.int32, (24, 128), 1)

    def to_row(v):
        return jnp.sum(jnp.where(diagonal, v, 0.0), axis=0, keepdims=True)

    part_a[plane_slot] = to_row(jnp.sum(jnp.concatenate([sums[0], sums[1], sums[2]], axis=0), axis=1, keepdims=True))

    def plane_copy(k):
        slot, device = plane_mate(k)
        return slot, pltpu.make_async_remote_copy(
            src_ref=part_a.at[plane_slot], dst_ref=part_a.at[plane_slot],
            send_sem=a_send.at[slot], recv_sem=a_recv.at[plane_slot],
            device_id=device, device_id_type=MESH,
        )

    def plane_wait(k):
        slot, device = plane_mate(k)
        return pltpu.make_async_remote_copy(
            src_ref=part_a.at[slot], dst_ref=part_a.at[slot],
            send_sem=a_send.at[slot], recv_sem=a_recv.at[slot],
            device_id=device, device_id_type=MESH,
        )

    def start_plane(k, carry):
        plane_copy(k)[1].start()
        return carry

    def finish_plane(k, carry):
        plane_wait(k).wait_recv()
        return carry

    lax.fori_loop(1, 32, start_plane, 0)
    lax.fori_loop(1, 32, finish_plane, 0)
    part_b[z] = jnp.sum(part_a[...], axis=0)
    line = []
    for k in range(1, 8):
        slot, device = line_mate(k)
        copy = pltpu.make_async_remote_copy(
            src_ref=part_b.at[z], dst_ref=part_b.at[z],
            send_sem=b_send.at[slot], recv_sem=b_recv.at[z],
            device_id=device, device_id_type=MESH,
        )
        copy.start()
        line.append((slot, device))
    for slot, device in line:
        pltpu.make_async_remote_copy(
            src_ref=part_b.at[slot], dst_ref=part_b.at[slot],
            send_sem=b_send.at[slot], recv_sem=b_recv.at[slot],
            device_id=device, device_id_type=MESH,
        ).wait_recv()
    total = jnp.sum(part_b[...], axis=0)
    nu = jnp.sum(jnp.where(diagonal, total, 0.0), axis=1, keepdims=True)
    predicted, corrected = recurrences(jnp.broadcast_to(nu, (24, 128)))

    upper = jnp.where(c == 1, 1.0, 0.0).astype(F32)
    away = [corrected[k : k + 1] + upper * (predicted[k : k + 1] - corrected[k : k + 1]) for k in range(12)]
    home = [predicted[k : k + 1] + upper * (corrected[k : k + 1] - predicted[k : k + 1]) for k in range(12)]

    def combine(ref, weights):
        spread = [jnp.broadcast_to(w, (8, 128)) for w in weights]

        def body(x):
            for h in range(2):
                for t in range(2):
                    at = pl.ds(8 + 8 * t, 8)
                    terms = [spread[k] * (u0, u1, u2, u3)[k % 4][k // 4, x + 4, h, at] for k in range(12)]
                    terms.append(init[x + 1, h, at])
                    while len(terms) > 1:
                        terms = [a + b for a, b in zip(terms[::2], terms[1::2])] + terms[len(terms) & ~1 :]
                    ref[h, x, pl.ds(8 * t, 8)] = terms[0]

        planes(0, 16, 4, body)

    def place(h, part):
        return out_hbm.at[0, pl.ds(part * 16, 16), :, pl.ds(128 * h, 128)]

    combine(theirs, away)
    gifts = [remote(theirs.at[h], place(h, c), out_send.at[h], out_recv.at[h], "near") for h in range(2)]
    for copy in gifts:
        copy.start()
    combine(mine, home)
    keeps = [pltpu.make_async_copy(mine.at[h], place(h, c), out_sem.at[h]) for h in range(2)]
    for copy in keeps:
        copy.start()

    sent(edges)
    for e, ref in enumerate((diag, u0.at[0], u0.at[1], u0.at[2])):
        sent(exchange(e, ref))
    for copy in gifts:
        copy.wait_send()

    def drain(k, carry):
        plane_wait(k).wait_send()
        return carry

    lax.fori_loop(1, 32, drain, 0)
    for slot, device in line:
        pltpu.make_async_remote_copy(
            src_ref=part_b.at[z], dst_ref=part_b.at[z],
            send_sem=b_send.at[slot], recv_sem=b_recv.at[slot],
            device_id=device, device_id_type=MESH,
        ).wait_send()
    for copy in keeps:
        copy.wait()
    for h in range(2):
        remote(theirs.at[h], place(h, other), out_send.at[h], out_recv.at[h], "near").wait_recv()


def per_device(init_field, source, damping):
    anywhere = pl.BlockSpec(memory_space=pl.ANY)
    dma = pltpu.SemaphoreType.DMA
    return pl.pallas_call(
        kernel,
        out_shape=jax.ShapeDtypeStruct((1, 32, 16, 256), F32),
        in_specs=[anywhere] * 3,
        out_specs=anywhere,
        scratch_shapes=[
            pltpu.VMEM((4, 24, 2, 32, 128), F32),
            pltpu.VMEM((3, 24, 2, 32, 128), F32),
            pltpu.VMEM((3, 24, 2, 32, 128), F32),
            pltpu.VMEM((3, 24, 2, 32, 128), F32),
            pltpu.VMEM((24, 2, 32, 128), F32),
            pltpu.VMEM((18, 2, 32, 128), F32),
            pltpu.VMEM((16, 2, 16, 128), F32),
            pltpu.VMEM((16, 2, 16, 128), F32),
            pltpu.VMEM((5, 2, 16, 2, 4, 128), F32),
            pltpu.VMEM((4, 2, 24, 2, 4, 128), F32),
            pltpu.VMEM((2, 16, 2, 1, 128), F32),
            pltpu.VMEM((2, 16, 2, 1, 128), F32),
            pltpu.VMEM((3, 8, 128), F32),
            pltpu.VMEM((32, 1, 128), F32),
            pltpu.VMEM((8, 1, 128), F32),
            pltpu.VMEM((2, 16, 16, 128), F32),
            pltpu.VMEM((2, 16, 16, 128), F32),
            dma((8,)), dma((3,)), dma((3,)), dma((4, 8)), dma((4, 8)),
            dma((32,)), dma((32,)), dma((8,)), dma((8,)), dma((2,)), dma((2,)), dma((2,)),
        ],
        compiler_params=pltpu.CompilerParams(collective_id=0, has_side_effects=True),
        cost_estimate=pl.CostEstimate(flops=50_000_000, bytes_accessed=3_000_000, transcendentals=0),
    )(init_field, source, damping)


def solution(mesh):
    block = P("gx", "yz", None)
    return jax.shard_map(
        per_device,
        mesh=mesh,
        in_specs=(block, block, block),
        out_specs=P("level", "gx", "yz", None),
        check_vma=False,
    )
```

```python
import functools

import jax
import jax.numpy as jnp
import numpy as np
from jax import lax
from jax.experimental import pallas as pl
from jax.experimental.pallas import tpu as pltpu
from jax.sharding import PartitionSpec as P

STEPS = 3
ITERS = 3
MESH = pl.DeviceIdType.MESH
F32 = jnp.float32

LOW, HIGH = 1.05, 15.0
MID, HALF = (LOW + HIGH) / 2, (HIGH - LOW) / 2
W = 4
STEP_PLANES = ((1, 22), (2, 20), (3, 18))


def block_polynomial():
    cheb = np.polynomial.chebyshev
    low, high = 2.0, 13.5

    def third(lam):
        x = (lam - (low + high) / 2) / ((high - low) / 2)
        return 4 * x**3 - 3 * x

    nodes = np.cos(np.pi * (np.arange(4) + 0.5) / 4)
    lam = MID + HALF * nodes
    rho = cheb.chebfit(nodes, (1 + (lam - 1) * third(lam) / third(0.0)) / lam, 3)
    return [float(c) for c in cheb.chebmul(rho, [0.0, 1.0])]


PSI = block_polynomial()


def planes(start, count, step, body):
    def turn(i, carry):
        for u in range(step):
            body(start + i * step + u)
        return carry

    lax.fori_loop(0, count // step, turn, 0)


def tree(terms):
    while len(terms) > 1:
        terms = [a + b for a, b in zip(terms[::2], terms[1::2])] + terms[len(terms) & ~1 :]
    return terms[0]


def zsum(v0, v1, first, last):
    a0, a1 = pltpu.roll(v0, 1, 1), pltpu.roll(v1, 1, 1)
    b0, b1 = pltpu.roll(v0, 127, 1), pltpu.roll(v1, 127, 1)
    n0 = jnp.where(first, 0.0, a0) + jnp.where(last, b1, b0)
    n1 = jnp.where(first, a0, a1) + jnp.where(last, 0.0, b1)
    return n0, n1


def recurrences(nu):
    c0, c1, c2, c3, c4 = PSI

    def pattern(rows, values):
        j = lax.rem(lax.broadcasted_iota(jnp.int32, (rows, 128), 0), 4)
        out = jnp.full((rows, 128), values[3], F32)
        for q in range(3):
            out = jnp.where(j == q, values[q], out)
        return out

    bands = {
        1: (1.0, 0.5, 0.5, 0.5 / c4),
        -1: (0.0, 0.5, 0.5, 0.5 - 0.5 * c2 / c4),
        0: (0.0, 0.0, 0.0, -0.5 * c3 / c4),
        -2: (0.0, 0.0, 0.0, -0.5 * c1 / c4),
        -3: (0.0, 0.0, 0.0, -0.5 * c0 / c4),
    }
    long = {o: pattern(24, v) for o, v in bands.items()}
    short = {o: pattern(16, v) for o, v in bands.items()}

    def shifted(v, o):
        rows = v.shape[0]
        return v if o % rows == 0 else pltpu.roll(v, o % rows, 0)

    def times(z, shift):
        f, m = z
        fx = sum(shifted(f * short[o], o) for o in bands)
        mx = sum(long[o] * shifted(m, -o) for o in bands)
        return fx + shift * f, mx + shift * m

    def inner(y, z):
        return jnp.sum(y[0] * z[1][:16], axis=0, keepdims=True)

    def axpy(y, s, z):
        return y[0] + s * z[0], y[1] + s * z[1]

    one = jnp.where(lax.broadcasted_iota(jnp.int32, (16, 128), 0) == 0, 1.0, 0.0).astype(F32)
    start = (one, nu)

    def solve(resid, answer):
        direction = resid
        norm = inner(resid, resid)
        for step in range(ITERS):
            image = times(direction, MID / HALF)
            alpha = norm / inner(direction, image)
            answer = axpy(answer, alpha, direction) if answer else (alpha * direction[0], alpha * direction[1])
            if step + 1 < ITERS:
                resid = axpy(resid, -alpha, image)
                following = inner(resid, resid)
                direction = axpy(resid, following / norm, direction)
                norm = following
        return answer

    back = (MID - 1.0) / HALF
    states = [None]
    corrected = None
    for step in range(STEPS):
        state = states[-1]
        resid = axpy(start, -1.0, times(state, back)) if state else start
        states.append(solve(resid, state))
        change = axpy(states[-1], -1.0, state) if state else states[-1]
        inside = axpy(corrected, -0.5, change) if corrected else (-0.5 * change[0], -0.5 * change[1])
        resid = axpy(start, -1.0, times(inside, back))
        corrected = solve(resid, corrected)
    return states[-1][0] * (1.0 / HALF), corrected[0] * (1.0 / HALF)


def kernel(
    init_hbm, source_hbm, damping_hbm, out_hbm,
    u0, u1, u2, u3, diag, init, source, damping, ys, yr, ps, pr, sums, part_a, part_b, mine, theirs,
    local_sem, init_send, init_recv, ghost_send, ghost_recv,
    a_send, a_recv, b_send, b_recv, out_sem, out_send, out_recv,
):
    c = lax.axis_index("level")
    gx = lax.axis_index("gx")
    yz = lax.axis_index("yz")
    other = 1 - c
    beyond = lax.rem(gx + 2 * c + 3, 4)
    above, below = lax.rem(yz + 1, 32), lax.rem(yz + 31, 32)
    device_of = {
        "near": (other, gx, yz), "up": (c, gx, above), "down": (c, gx, below), "far": (other, beyond, yz),
        "near_up": (other, gx, above), "near_down": (other, gx, below),
        "far_up": (other, beyond, above), "far_down": (other, beyond, below),
    }
    y, z = lax.rem(yz, 4), lax.div(yz, 4)
    plane_slot = gx * 8 + c * 4 + y

    plane_mates = [
        (cc, xx, z * 4 + yy)
        for i, xx in enumerate([gx] + [lax.rem(gx + k, 4) for k in range(1, 4)])
        for j, cc in enumerate([c, other])
        for m, yy in enumerate([y] + [lax.rem(y + k, 4) for k in range(1, 4)])
        if i + j + m > 0
    ]
    line_mates = [(c, gx, lax.rem(z + k, 8) * 4 + y) for k in range(1, 8)]

    low_ok, high_ok = yz > 0, yz < 31
    x_low_ok, x_high_ok = gx + c > 0, gx + c < 4
    far_ok = jnp.logical_and(gx + 2 * c >= 1, gx + 2 * c <= 4)
    exists = {
        "near": None, "up": high_ok, "down": low_ok, "far": far_ok, "near_up": high_ok, "near_down": low_ok,
        "far_up": jnp.logical_and(far_ok, high_ok), "far_down": jnp.logical_and(far_ok, low_ok),
    }

    def where_there(name, act):
        if exists[name] is None:
            act()
        else:
            pl.when(exists[name])(act)
    own = pl.ds(c * 16, 16)
    rows = pl.ds(8, 16)
    loads = []
    for h in range(2):
        s = pl.ds(128 * h, 128)
        loads += [
            pltpu.make_async_copy(damping_hbm.at[own, :, s], damping.at[:, h], local_sem.at[h]),
            pltpu.make_async_copy(init_hbm.at[own, :, s], init.at[pl.ds(1, 16), h, rows], local_sem.at[2 + h]),
            pltpu.make_async_copy(
                init_hbm.at[pl.ds(16 - c, 1), :, s], init.at[pl.ds(17 - 17 * c, 1), h, rows], local_sem.at[4 + h]
            ),
            pltpu.make_async_copy(source_hbm.at[own, :, s], source.at[:, h], local_sem.at[6 + h]),
        ]
    for load in loads:
        load.start()

    barrier = pltpu.get_barrier_semaphore()

    def greet(device):
        pl.semaphore_signal(barrier, inc=1, device_id=device, device_id_type=MESH)

    for device in line_mates:
        greet(device)
    greeted = 38
    for name, there in exists.items():
        where_there(
            name,
            functools.partial(greet, device_of[name]),
        )
        greeted = greeted + (1 if there is None else there.astype(jnp.int32))
    for device in plane_mates:
        greet(device)

    lane = lax.broadcasted_iota(jnp.int32, (8, 128), 1)
    sublane = lax.broadcasted_iota(jnp.int32, (8, 128), 0)
    first, last = lane == 0, lane == 127
    has_low, has_high = low_ok.astype(F32), high_ok.astype(F32)
    x_low, x_high = x_low_ok.astype(F32), x_high_ok.astype(F32)

    def edge_of(x):
        return jnp.where(x < 4, x_low, jnp.where(x >= 20, x_high, 1.0))

    def remote(src, dst, sends, recvs, name):
        return pltpu.make_async_remote_copy(
            src_ref=src, dst_ref=dst, send_sem=sends, recv_sem=recvs,
            device_id=device_of[name], device_id_type=MESH,
        )

    def exchange(e, ref):
        slab, into = ys.at[e], yr.at[e]
        plan = (
            (slab.at[1], into.at[0, pl.ds(4, 16)], "up"),
            (slab.at[0], into.at[1, pl.ds(4, 16)], "down"),
            (ref.at[pl.ds(4 + 12 * c, 4), :, rows], ref.at[pl.ds(20 - 20 * c, 4), :, rows], "far"),
            (slab.at[1, pl.ds(13 * c, 3)], into.at[0, pl.ds(20 - 19 * c, 3)], "far_up"),
            (slab.at[0, pl.ds(13 * c, 3)], into.at[1, pl.ds(20 - 19 * c, 3)], "far_down"),
            (slab.at[1, pl.ds(13 - 13 * c, 3)], into.at[0, pl.ds(1 + 19 * c, 3)], "near_up"),
            (slab.at[0, pl.ds(13 - 13 * c, 3)], into.at[1, pl.ds(1 + 19 * c, 3)], "near_down"),
            (ref.at[pl.ds(16 - 12 * c, 4), :, rows], ref.at[pl.ds(20 * c, 4), :, rows], "near"),
        )
        return [
            (name, remote(src, dst, ghost_send.at[e, i], ghost_recv.at[e, i], name))
            for i, (src, dst, name) in enumerate(plan)
        ]

    def launch(copies):
        for name, copy in copies:
            where_there(name, copy.start)

    def receive(copies):
        for name, copy in copies:
            turned = name.replace("up", "down") if "up" in name else name.replace("down", "up")
            where_there(turned, copy.wait_recv)

    def sent(copies):
        for name, copy in copies:
            where_there(name, copy.wait_send)

    for load in loads:
        load.wait()

    def prepare(x):
        for h in range(2):
            for t in range(2):
                at = pl.ds(8 * t, 8)
                d = (damping[x, h, at] + (7.0 - MID)) * (2.0 / HALF)
                diag[x + 4, h, pl.ds(8 + 8 * t, 8)] = d
                ys[0, t, x, h] = d[4 * t : 4 * t + 4]
            ps[0, x, h] = init[x + 1, h, 8:9]
            ps[1, x, h] = init[x + 1, h, 23:24]

    planes(0, 16, 4, prepare)
    pl.semaphore_wait(barrier, greeted)
    edges = [
        ("up", remote(ps.at[1], pr.at[0], init_send.at[0], init_recv.at[0], "up")),
        ("down", remote(ps.at[0], pr.at[1], init_send.at[1], init_recv.at[1], "down")),
        ("far", remote(
            init.at[pl.ds(1 + 15 * c, 1), :, rows], init.at[pl.ds(17 - 17 * c, 1), :, rows],
            init_send.at[2], init_recv.at[2], "far",
        )),
    ]
    launch(edges)
    launch(exchange(0, diag))
    receive(edges)
    for h in range(2):
        init[0, h, rows] = jnp.where(x_low_ok, init[0, h, rows], 0.0)
        init[17, h, rows] = jnp.where(x_high_ok, init[17, h, rows], 0.0)

    def neighbours_of(ref, x, at):
        v = [ref[x, h, pl.ds(at, 8)] for h in range(2)]
        n = zsum(*v, first, last)
        total = []
        for h in range(2):
            along_y = ref[x, h, pl.ds(at - 1, 8)] + ref[x, h, pl.ds(at + 1, 8)]
            total.append(n[h] + (along_y + (ref[x - 1, h, pl.ds(at, 8)] + ref[x + 1, h, pl.ds(at, 8)])))
        return v, total

    def edge_rows(x):
        for h in range(2):
            init[x + 1, h, 7:8] = jnp.where(low_ok, pr[0, x, h], 0.0)
            init[x + 1, h, 24:25] = jnp.where(high_ok, pr[1, x, h], 0.0)

    planes(0, 16, 4, edge_rows)

    def first_vector(x):
        for t in range(2):
            v, total = neighbours_of(init, x + 1, 8 + 8 * t)
            for h in range(2):
                at = pl.ds(8 * t, 8)
                w = source[x, h, at] - ((damping[x, h, at] + 6.0) * v[h] - total[h])
                u0[0, x + 4, h, pl.ds(8 + 8 * t, 8)] = w
                ys[1, t, x, h] = w[4 * t : 4 * t + 4]

    planes(0, 16, 4, first_vector)
    launch(exchange(1, u0.at[0]))

    def merge(e, ref):
        receive(exchange(e, ref))

        def ghosts(x):
            x_in = jnp.logical_and(jnp.logical_or(x >= 4, x_low_ok), jnp.logical_or(x < 20, x_high_ok))
            low_in, high_in = jnp.logical_and(low_ok, x_in), jnp.logical_and(high_ok, x_in)
            for h in range(2):
                ref[x, h, 4:8] = jnp.where(low_in, yr[e, 0, x, h], 0.0)
                ref[x, h, 24:28] = jnp.where(high_in, yr[e, 1, x, h], 0.0)

        planes(0, 24, 4, ghosts)
        for x in range(4):
            for h in range(2):
                ref[x, h, rows] = jnp.where(x_low_ok, ref[x, h, rows], 0.0)
                ref[20 + x, h, rows] = jnp.where(x_high_ok, ref[20 + x, h, rows], 0.0)

    merge(0, diag)

    def block_of(block, carry):
        basis = [u.at[block] for u in (u0, u1, u2, u3)]
        following = u0.at[block + 1]
        merge(block + 1, basis[0])
        for j, step in STEP_PLANES:
            starts = (4 + j, 12 + j, 20 - j)
            keep = []
            for at in starts:
                r = sublane + at
                keep.append(jnp.where(r < 8, has_low, jnp.where(r >= 24, has_high, 1.0)).astype(F32))

            def apply(x, j=j, starts=starts, keep=keep):
                edge = edge_of(x)
                for at, mask in zip(starts, keep):
                    v, total = neighbours_of(basis[j - 1], x, at)
                    for h in range(2):
                        t = diag[x, h, pl.ds(at, 8)] * v[h] - total[h] * (2.0 / HALF)
                        t = 0.5 * t if j == 1 else t - basis[j - 2][x, h, pl.ds(at, 8)]
                        basis[j][x, h, pl.ds(at, 8)] = t * (mask * edge)

            planes(j, 24 - 2 * j, step, apply)

        def close(i, carry):
            done = []
            for u in range(16):
                x = 16 * i + u + 4
                for at in (8, 16):
                    v, total = neighbours_of(basis[3], x, at)
                    for h in range(2):
                        old = [basis[q][x, h, pl.ds(at, 8)] for q in range(3)]
                        new = diag[x, h, pl.ds(at, 8)] * v[h] - total[h] * (2.0 / HALF) - old[2]
                        new = PSI[4] * new + (PSI[3] * v[h] + PSI[2] * old[2]) + (PSI[1] * old[1] + PSI[0] * old[0])
                        done.append((x, h, at, new))
            for x, h, at, new in done:
                following[x, h, pl.ds(at, 8)] = new
                t = at // 8 - 1
                ys[block + 2, t, x - 4, h] = new[4 * t : 4 * t + 4]
            return carry

        lax.fori_loop(0, 1, close, 0)

        @pl.when(block < 2)
        def _():
            launch(exchange(block + 2, following))

        def products(i, carry):
            gathered = [[] for _ in range(8)]
            for u in range(4):
                for h in range(2):
                    for t in range(2):
                        v = [f[4 * i + u + 4, h, pl.ds(8 + 8 * t, 8)] for f in (*basis, following)]
                        for q in range(4):
                            gathered[q].append(v[0] * v[q])
                            gathered[4 + q].append(v[4] * v[q])
            return tuple(a + tree(terms) for a, terms in zip(carry, gathered))

        totals = lax.fori_loop(0, 4, products, (jnp.zeros((8, 128), F32),) * 8)
        for q, total in enumerate(totals):
            sums[block, q : q + 1] = jnp.sum(total, axis=0, keepdims=True)
        return carry

    lax.fori_loop(0, 3, block_of, 0)

    diagonal = lax.broadcasted_iota(jnp.int32, (24, 128), 0) == lax.broadcasted_iota(jnp.int32, (24, 128), 1)

    def to_row(v):
        return jnp.sum(jnp.where(diagonal, v, 0.0), axis=0, keepdims=True)

    part_a[plane_slot] = to_row(jnp.sum(jnp.concatenate([sums[0], sums[1], sums[2]], axis=0), axis=1, keepdims=True))

    def share(part, slot, sends, recvs, devices):
        for device in devices:
            pltpu.make_async_remote_copy(
                src_ref=part.at[slot], dst_ref=part.at[slot], send_sem=sends, recv_sem=recvs,
                device_id=device, device_id_type=MESH,
            ).start()

    def settle(part, sem):
        rest = part.at[pl.ds(0, part.shape[0] - 1)]
        pltpu.make_async_copy(rest, rest, sem).wait()

    share(part_a, plane_slot, a_send, a_recv, plane_mates)
    settle(part_a, a_recv)
    part_b[z] = jnp.sum(part_a[...], axis=0)
    share(part_b, z, b_send, b_recv, line_mates)
    settle(part_b, b_recv)
    total = jnp.sum(part_b[...], axis=0)
    nu = jnp.sum(jnp.where(diagonal, total, 0.0), axis=1, keepdims=True)
    predicted, corrected = recurrences(jnp.broadcast_to(nu, (24, 128)))

    upper = jnp.where(c == 1, 1.0, 0.0).astype(F32)
    away = [corrected[k : k + 1] + upper * (predicted[k : k + 1] - corrected[k : k + 1]) for k in range(12)]
    home = [predicted[k : k + 1] + upper * (corrected[k : k + 1] - predicted[k : k + 1]) for k in range(12)]

    away = [jnp.broadcast_to(w, (8, 128)) for w in away]
    home = [jnp.broadcast_to(w, (8, 128)) for w in home]

    def combine(ref, h, weights):
        def body(x):
            for t in range(2):
                at = pl.ds(8 + 8 * t, 8)
                terms = [weights[k] * (u0, u1, u2, u3)[k % 4][k // 4, x + 4, h, at] for k in range(12)]
                ref[h, x, pl.ds(8 * t, 8)] = tree([init[x + 1, h, at]] + terms)

        planes(0, 16, 8, body)

    def place(h, part):
        return out_hbm.at[0, pl.ds(part * 16, 16), :, pl.ds(128 * h, 128)]

    gifts, keeps = [], []
    for h in range(2):
        combine(theirs, h, away)
        gifts.append(remote(theirs.at[h], place(h, c), out_send.at[h], out_recv.at[h], "near"))
        gifts[-1].start()
    for h in range(2):
        combine(mine, h, home)
        keeps.append(pltpu.make_async_copy(mine.at[h], place(h, c), out_sem.at[h]))
        keeps[-1].start()

    sent(edges)
    for e, ref in enumerate((diag, u0.at[0], u0.at[1], u0.at[2])):
        sent(exchange(e, ref))
    for copy in gifts:
        copy.wait_send()

    settle(part_a, a_send)
    settle(part_b, b_send)
    for copy in keeps:
        copy.wait()
    for h in range(2):
        remote(theirs.at[h], place(h, other), out_send.at[h], out_recv.at[h], "near").wait_recv()


def per_device(init_field, source, damping):
    anywhere = pl.BlockSpec(memory_space=pl.ANY)
    dma = pltpu.SemaphoreType.DMA
    return pl.pallas_call(
        kernel,
        out_shape=jax.ShapeDtypeStruct((1, 32, 16, 256), F32),
        in_specs=[anywhere] * 3,
        out_specs=anywhere,
        scratch_shapes=[
            pltpu.VMEM((4, 24, 2, 32, 128), F32),
            pltpu.VMEM((3, 24, 2, 32, 128), F32),
            pltpu.VMEM((3, 24, 2, 32, 128), F32),
            pltpu.VMEM((3, 24, 2, 32, 128), F32),
            pltpu.VMEM((24, 2, 32, 128), F32),
            pltpu.VMEM((18, 2, 32, 128), F32),
            pltpu.VMEM((16, 2, 16, 128), F32),
            pltpu.VMEM((16, 2, 16, 128), F32),
            pltpu.VMEM((5, 2, 16, 2, 4, 128), F32),
            pltpu.VMEM((4, 2, 24, 2, 4, 128), F32),
            pltpu.VMEM((2, 16, 2, 1, 128), F32),
            pltpu.VMEM((2, 16, 2, 1, 128), F32),
            pltpu.VMEM((3, 8, 128), F32),
            pltpu.VMEM((32, 1, 128), F32),
            pltpu.VMEM((8, 1, 128), F32),
            pltpu.VMEM((2, 16, 16, 128), F32),
            pltpu.VMEM((2, 16, 16, 128), F32),
            dma((8,)), dma((3,)), dma((3,)), dma((4, 8)), dma((4, 8)),
            dma, dma, dma, dma, dma((2,)), dma((2,)), dma((2,)),
        ],
        compiler_params=pltpu.CompilerParams(collective_id=0, has_side_effects=True),
        cost_estimate=pl.CostEstimate(flops=50_000_000, bytes_accessed=3_000_000, transcendentals=0),
    )(init_field, source, damping)


def solution(mesh):
    block = P("gx", "yz", None)
    return jax.shard_map(
        per_device,
        mesh=mesh,
        in_specs=(block, block, block),
        out_specs=P("level", "gx", "yz", None),
        check_vma=False,
    )
```

```python
import functools

import jax
import jax.numpy as jnp
import numpy as np
from jax import lax
from jax.experimental import pallas as pl
from jax.experimental.pallas import tpu as pltpu
from jax.sharding import PartitionSpec as P

STEPS = 3
ITERS = 3
MESH = pl.DeviceIdType.MESH
F32 = jnp.float32

LOW, HIGH = 1.05, 15.0
MID, HALF = (LOW + HIGH) / 2, (HIGH - LOW) / 2
W = 4
STEP_PLANES = ((1, 22), (2, 20), (3, 18))


def block_polynomial():
    cheb = np.polynomial.chebyshev
    low, high = 2.0, 13.5

    def third(lam):
        x = (lam - (low + high) / 2) / ((high - low) / 2)
        return 4 * x**3 - 3 * x

    nodes = np.cos(np.pi * (np.arange(4) + 0.5) / 4)
    lam = MID + HALF * nodes
    rho = cheb.chebfit(nodes, (1 + (lam - 1) * third(lam) / third(0.0)) / lam, 3)
    return [float(c) for c in cheb.chebmul(rho, [0.0, 1.0])]


PSI = block_polynomial()


def planes(start, count, step, body):
    def turn(i, carry):
        for u in range(step):
            body(start + i * step + u)
        return carry

    lax.fori_loop(0, count // step, turn, 0)


def tree(terms):
    while len(terms) > 1:
        terms = [a + b for a, b in zip(terms[::2], terms[1::2])] + terms[len(terms) & ~1 :]
    return terms[0]


def zsum(v0, v1, first, last):
    a0, a1 = pltpu.roll(v0, 1, 1), pltpu.roll(v1, 1, 1)
    b0, b1 = pltpu.roll(v0, 127, 1), pltpu.roll(v1, 127, 1)
    n0 = jnp.where(first, 0.0, a0) + jnp.where(last, b1, b0)
    n1 = jnp.where(first, a0, a1) + jnp.where(last, 0.0, b1)
    return n0, n1


def recurrences(nu):
    c0, c1, c2, c3, c4 = PSI

    def pattern(rows, values):
        j = lax.rem(lax.broadcasted_iota(jnp.int32, (rows, 128), 0), 4)
        out = jnp.full((rows, 128), values[3], F32)
        for q in range(3):
            out = jnp.where(j == q, values[q], out)
        return out

    bands = {
        1: (1.0, 0.5, 0.5, 0.5 / c4),
        -1: (0.0, 0.5, 0.5, 0.5 - 0.5 * c2 / c4),
        0: (0.0, 0.0, 0.0, -0.5 * c3 / c4),
        -2: (0.0, 0.0, 0.0, -0.5 * c1 / c4),
        -3: (0.0, 0.0, 0.0, -0.5 * c0 / c4),
    }
    long = {o: pattern(24, v) for o, v in bands.items()}
    short = {o: pattern(16, v) for o, v in bands.items()}

    def shifted(v, o):
        rows = v.shape[0]
        return v if o % rows == 0 else pltpu.roll(v, o % rows, 0)

    def times(z, shift):
        f, m = z
        fx = sum(shifted(f * short[o], o) for o in bands)
        mx = sum(long[o] * shifted(m, -o) for o in bands)
        return fx + shift * f, mx + shift * m

    def inner(y, z):
        return jnp.sum(y[0] * z[1][:16], axis=0, keepdims=True)

    def axpy(y, s, z):
        return y[0] + s * z[0], y[1] + s * z[1]

    one = jnp.where(lax.broadcasted_iota(jnp.int32, (16, 128), 0) == 0, 1.0, 0.0).astype(F32)
    start = (one, nu)

    def solve(resid, answer):
        direction = resid
        norm = inner(resid, resid)
        for step in range(ITERS):
            image = times(direction, MID / HALF)
            alpha = norm / inner(direction, image)
            answer = axpy(answer, alpha, direction) if answer else (alpha * direction[0], alpha * direction[1])
            if step + 1 < ITERS:
                resid = axpy(resid, -alpha, image)
                following = inner(resid, resid)
                direction = axpy(resid, following / norm, direction)
                norm = following
        return answer

    back = (MID - 1.0) / HALF
    states = [None]
    corrected = None
    for step in range(STEPS):
        state = states[-1]
        resid = axpy(start, -1.0, times(state, back)) if state else start
        states.append(solve(resid, state))
        change = axpy(states[-1], -1.0, state) if state else states[-1]
        inside = axpy(corrected, -0.5, change) if corrected else (-0.5 * change[0], -0.5 * change[1])
        resid = axpy(start, -1.0, times(inside, back))
        corrected = solve(resid, corrected)
    return states[-1][0] * (1.0 / HALF), corrected[0] * (1.0 / HALF)


def kernel(
    init_hbm, source_hbm, damping_hbm, out_hbm,
    u0, u1, u2, u3, diag, init, source, damping, ys, yr, ps, pr, sums, part_a, part_b, mine, theirs,
    local_sem, init_send, init_recv, ghost_send, ghost_recv,
    a_send, a_recv, b_send, b_recv, out_sem, out_send, out_recv,
):
    c = lax.axis_index("level")
    gx = lax.axis_index("gx")
    yz = lax.axis_index("yz")
    other = 1 - c
    beyond = lax.rem(gx + 2 * c + 3, 4)
    above, below = lax.rem(yz + 1, 32), lax.rem(yz + 31, 32)
    device_of = {
        "near": (other, gx, yz), "up": (c, gx, above), "down": (c, gx, below), "far": (other, beyond, yz),
        "near_up": (other, gx, above), "near_down": (other, gx, below),
        "far_up": (other, beyond, above), "far_down": (other, beyond, below),
    }
    y, z = lax.rem(yz, 4), lax.div(yz, 4)
    plane_slot = gx * 8 + c * 4 + y

    plane_mates = [
        (cc, xx, z * 4 + yy)
        for i, xx in enumerate([gx] + [lax.rem(gx + k, 4) for k in range(1, 4)])
        for j, cc in enumerate([c, other])
        for m, yy in enumerate([y] + [lax.rem(y + k, 4) for k in range(1, 4)])
        if i + j + m > 0
    ]
    line_mates = [(c, gx, lax.rem(z + k, 8) * 4 + y) for k in range(1, 8)]

    low_ok, high_ok = yz > 0, yz < 31
    x_low_ok, x_high_ok = gx + c > 0, gx + c < 4
    far_ok = jnp.logical_and(gx + 2 * c >= 1, gx + 2 * c <= 4)
    exists = {
        "near": None, "up": high_ok, "down": low_ok, "far": far_ok, "near_up": high_ok, "near_down": low_ok,
        "far_up": jnp.logical_and(far_ok, high_ok), "far_down": jnp.logical_and(far_ok, low_ok),
    }

    def where_there(name, act):
        if exists[name] is None:
            act()
        else:
            pl.when(exists[name])(act)
    barrier = pltpu.get_barrier_semaphore()

    def greet(device):
        pl.semaphore_signal(barrier, inc=1, device_id=device, device_id_type=MESH)

    for device in plane_mates:
        greet(device)
    greeted = 38
    own = pl.ds(c * 16, 16)
    rows = pl.ds(8, 16)
    loads = []
    for h in range(2):
        s = pl.ds(128 * h, 128)
        loads += [
            pltpu.make_async_copy(damping_hbm.at[own, :, s], damping.at[:, h], local_sem.at[h]),
            pltpu.make_async_copy(init_hbm.at[own, :, s], init.at[pl.ds(1, 16), h, rows], local_sem.at[2 + h]),
            pltpu.make_async_copy(
                init_hbm.at[pl.ds(16 - c, 1), :, s], init.at[pl.ds(17 - 17 * c, 1), h, rows], local_sem.at[4 + h]
            ),
            pltpu.make_async_copy(source_hbm.at[own, :, s], source.at[:, h], local_sem.at[6 + h]),
        ]
    for load in loads:
        load.start()

    for name, there in exists.items():
        where_there(
            name,
            functools.partial(greet, device_of[name]),
        )
        greeted = greeted + (1 if there is None else there.astype(jnp.int32))
    for device in line_mates:
        greet(device)

    lane = lax.broadcasted_iota(jnp.int32, (8, 128), 1)
    sublane = lax.broadcasted_iota(jnp.int32, (8, 128), 0)
    first, last = lane == 0, lane == 127
    has_low, has_high = low_ok.astype(F32), high_ok.astype(F32)
    x_low, x_high = x_low_ok.astype(F32), x_high_ok.astype(F32)

    def edge_of(x):
        return jnp.where(x < 4, x_low, jnp.where(x >= 20, x_high, 1.0))

    def remote(src, dst, sends, recvs, name):
        return pltpu.make_async_remote_copy(
            src_ref=src, dst_ref=dst, send_sem=sends, recv_sem=recvs,
            device_id=device_of[name], device_id_type=MESH,
        )

    def exchange(e, ref):
        slab, into = ys.at[e], yr.at[e]
        plan = (
            (slab.at[1], into.at[0, pl.ds(4, 16)], "up"),
            (slab.at[0], into.at[1, pl.ds(4, 16)], "down"),
            (ref.at[pl.ds(4 + 12 * c, 4), :, rows], ref.at[pl.ds(20 - 20 * c, 4), :, rows], "far"),
            (slab.at[1, pl.ds(13 * c, 3)], into.at[0, pl.ds(20 - 19 * c, 3)], "far_up"),
            (slab.at[0, pl.ds(13 * c, 3)], into.at[1, pl.ds(20 - 19 * c, 3)], "far_down"),
            (slab.at[1, pl.ds(13 - 13 * c, 3)], into.at[0, pl.ds(1 + 19 * c, 3)], "near_up"),
            (slab.at[0, pl.ds(13 - 13 * c, 3)], into.at[1, pl.ds(1 + 19 * c, 3)], "near_down"),
            (ref.at[pl.ds(16 - 12 * c, 4), :, rows], ref.at[pl.ds(20 * c, 4), :, rows], "near"),
        )
        return [
            (name, remote(src, dst, ghost_send.at[e, i], ghost_recv.at[e, i], name))
            for i, (src, dst, name) in enumerate(plan)
        ]

    def launch(copies):
        for name, copy in copies:
            where_there(name, copy.start)

    def receive(copies):
        for name, copy in copies:
            turned = name.replace("up", "down") if "up" in name else name.replace("down", "up")
            where_there(turned, copy.wait_recv)

    def sent(copies):
        for name, copy in copies:
            where_there(name, copy.wait_send)

    for load in loads:
        load.wait()

    def prepare(x):
        for h in range(2):
            for t in range(2):
                at = pl.ds(8 * t, 8)
                d = (damping[x, h, at] + (7.0 - MID)) * (2.0 / HALF)
                diag[x + 4, h, pl.ds(8 + 8 * t, 8)] = d
                ys[0, t, x, h] = d[4 * t : 4 * t + 4]
            ps[0, x, h] = init[x + 1, h, 8:9]
            ps[1, x, h] = init[x + 1, h, 23:24]

    planes(0, 16, 8, prepare)
    pl.semaphore_wait(barrier, greeted)
    edges = [
        ("up", remote(ps.at[1], pr.at[0], init_send.at[0], init_recv.at[0], "up")),
        ("down", remote(ps.at[0], pr.at[1], init_send.at[1], init_recv.at[1], "down")),
        ("far", remote(
            init.at[pl.ds(1 + 15 * c, 1), :, rows], init.at[pl.ds(17 - 17 * c, 1), :, rows],
            init_send.at[2], init_recv.at[2], "far",
        )),
    ]
    launch(edges)
    launch(exchange(0, diag))
    receive(edges)
    for h in range(2):
        init[0, h, rows] = jnp.where(x_low_ok, init[0, h, rows], 0.0)
        init[17, h, rows] = jnp.where(x_high_ok, init[17, h, rows], 0.0)

    def neighbours_of(ref, x, at):
        v = [ref[x, h, pl.ds(at, 8)] for h in range(2)]
        n = zsum(*v, first, last)
        total = []
        for h in range(2):
            along_y = ref[x, h, pl.ds(at - 1, 8)] + ref[x, h, pl.ds(at + 1, 8)]
            total.append(n[h] + (along_y + (ref[x - 1, h, pl.ds(at, 8)] + ref[x + 1, h, pl.ds(at, 8)])))
        return v, total

    def edge_rows(x):
        for h in range(2):
            init[x + 1, h, 7:8] = jnp.where(low_ok, pr[0, x, h], 0.0)
            init[x + 1, h, 24:25] = jnp.where(high_ok, pr[1, x, h], 0.0)

    planes(0, 16, 16, edge_rows)

    def first_vector(x):
        for t in range(2):
            v, total = neighbours_of(init, x + 1, 8 + 8 * t)
            for h in range(2):
                at = pl.ds(8 * t, 8)
                w = source[x, h, at] - ((damping[x, h, at] + 6.0) * v[h] - total[h])
                u0[0, x + 4, h, pl.ds(8 + 8 * t, 8)] = w
                ys[1, t, x, h] = w[4 * t : 4 * t + 4]

    planes(0, 16, 16, first_vector)
    launch(exchange(1, u0.at[0]))

    def merge(e, ref):
        receive(exchange(e, ref))

        def ghosts(x):
            x_in = jnp.logical_and(jnp.logical_or(x >= 4, x_low_ok), jnp.logical_or(x < 20, x_high_ok))
            low_in, high_in = jnp.logical_and(low_ok, x_in), jnp.logical_and(high_ok, x_in)
            for h in range(2):
                ref[x, h, 4:8] = jnp.where(low_in, yr[e, 0, x, h], 0.0)
                ref[x, h, 24:28] = jnp.where(high_in, yr[e, 1, x, h], 0.0)

        planes(0, 24, 12, ghosts)
        for x in range(4):
            for h in range(2):
                ref[x, h, rows] = jnp.where(x_low_ok, ref[x, h, rows], 0.0)
                ref[20 + x, h, rows] = jnp.where(x_high_ok, ref[20 + x, h, rows], 0.0)

    merge(0, diag)

    def block_of(block, carry):
        basis = [u.at[block] for u in (u0, u1, u2, u3)]
        following = u0.at[block + 1]
        merge(block + 1, basis[0])
        for j, step in STEP_PLANES:
            starts = (4 + j, 12 + j, 20 - j)
            keep = []
            for at in starts:
                r = sublane + at
                keep.append(jnp.where(r < 8, has_low, jnp.where(r >= 24, has_high, 1.0)).astype(F32))

            def apply(x, j=j, starts=starts, keep=keep):
                edge = edge_of(x)
                for at, mask in zip(starts, keep):
                    v, total = neighbours_of(basis[j - 1], x, at)
                    for h in range(2):
                        t = diag[x, h, pl.ds(at, 8)] * v[h] - total[h] * (2.0 / HALF)
                        t = 0.5 * t if j == 1 else t - basis[j - 2][x, h, pl.ds(at, 8)]
                        basis[j][x, h, pl.ds(at, 8)] = t * (mask * edge)

            planes(j, 24 - 2 * j, step, apply)

        def close(i, carry):
            done = []
            for u in range(16):
                x = 16 * i + u + 4
                for at in (8, 16):
                    v, total = neighbours_of(basis[3], x, at)
                    for h in range(2):
                        old = [basis[q][x, h, pl.ds(at, 8)] for q in range(3)]
                        new = diag[x, h, pl.ds(at, 8)] * v[h] - total[h] * (2.0 / HALF) - old[2]
                        new = PSI[4] * new + (PSI[3] * v[h] + PSI[2] * old[2]) + (PSI[1] * old[1] + PSI[0] * old[0])
                        done.append((x, h, at, new))
            for x, h, at, new in done:
                following[x, h, pl.ds(at, 8)] = new
                t = at // 8 - 1
                ys[block + 2, t, x - 4, h] = new[4 * t : 4 * t + 4]
            return carry

        lax.fori_loop(0, 1, close, 0)

        @pl.when(block < 2)
        def _():
            launch(exchange(block + 2, following))

        def products(i, carry):
            gathered = [[] for _ in range(8)]
            for u in range(4):
                for h in range(2):
                    for t in range(2):
                        v = [f[4 * i + u + 4, h, pl.ds(8 + 8 * t, 8)] for f in (*basis, following)]
                        for q in range(4):
                            gathered[q].append(v[0] * v[q])
                            gathered[4 + q].append(v[4] * v[q])
            return tuple(a + tree(terms) for a, terms in zip(carry, gathered))

        totals = lax.fori_loop(0, 4, products, (jnp.zeros((8, 128), F32),) * 8)
        for q, total in enumerate(totals):
            sums[block, q : q + 1] = jnp.sum(total, axis=0, keepdims=True)
        return carry

    lax.fori_loop(0, 3, block_of, 0)

    diagonal = lax.broadcasted_iota(jnp.int32, (24, 128), 0) == lax.broadcasted_iota(jnp.int32, (24, 128), 1)

    def to_row(v):
        return jnp.sum(jnp.where(diagonal, v, 0.0), axis=0, keepdims=True)

    part_a[plane_slot] = to_row(jnp.sum(jnp.concatenate([sums[0], sums[1], sums[2]], axis=0), axis=1, keepdims=True))

    def share(part, slot, sends, recvs, devices):
        for device in devices:
            pltpu.make_async_remote_copy(
                src_ref=part.at[slot], dst_ref=part.at[slot], send_sem=sends, recv_sem=recvs,
                device_id=device, device_id_type=MESH,
            ).start()

    def settle(part, sem):
        rest = part.at[pl.ds(0, part.shape[0] - 1)]
        pltpu.make_async_copy(rest, rest, sem).wait()

    share(part_a, plane_slot, a_send, a_recv, plane_mates)
    settle(part_a, a_recv)
    part_b[z] = jnp.sum(part_a[...], axis=0)
    share(part_b, z, b_send, b_recv, line_mates)
    settle(part_b, b_recv)
    total = jnp.sum(part_b[...], axis=0)
    nu = jnp.sum(jnp.where(diagonal, total, 0.0), axis=1, keepdims=True)
    predicted, corrected = recurrences(jnp.broadcast_to(nu, (24, 128)))

    upper = jnp.where(c == 1, 1.0, 0.0).astype(F32)
    away = [corrected[k : k + 1] + upper * (predicted[k : k + 1] - corrected[k : k + 1]) for k in range(12)]
    home = [predicted[k : k + 1] + upper * (corrected[k : k + 1] - predicted[k : k + 1]) for k in range(12)]

    away = [jnp.broadcast_to(w, (8, 128)) for w in away]
    home = [jnp.broadcast_to(w, (8, 128)) for w in home]

    def combine(ref, h, weights):
        def body(x):
            for t in range(2):
                at = pl.ds(8 + 8 * t, 8)
                terms = [weights[k] * (u0, u1, u2, u3)[k % 4][k // 4, x + 4, h, at] for k in range(12)]
                ref[h, x, pl.ds(8 * t, 8)] = tree([init[x + 1, h, at]] + terms)

        planes(0, 16, 8, body)

    def place(h, part):
        return out_hbm.at[0, pl.ds(part * 16, 16), :, pl.ds(128 * h, 128)]

    gifts, keeps = [], []
    for h in range(2):
        combine(theirs, h, away)
        gifts.append(remote(theirs.at[h], place(h, c), out_send.at[h], out_recv.at[h], "near"))
        gifts[-1].start()
    for h in range(2):
        combine(mine, h, home)
        keeps.append(pltpu.make_async_copy(mine.at[h], place(h, c), out_sem.at[h]))
        keeps[-1].start()

    sent(edges)
    for e, ref in enumerate((diag, u0.at[0], u0.at[1], u0.at[2])):
        sent(exchange(e, ref))
    for copy in gifts:
        copy.wait_send()

    settle(part_a, a_send)
    settle(part_b, b_send)
    for copy in keeps:
        copy.wait()
    for h in range(2):
        remote(theirs.at[h], place(h, other), out_send.at[h], out_recv.at[h], "near").wait_recv()


def per_device(init_field, source, damping):
    anywhere = pl.BlockSpec(memory_space=pl.ANY)
    dma = pltpu.SemaphoreType.DMA
    return pl.pallas_call(
        kernel,
        out_shape=jax.ShapeDtypeStruct((1, 32, 16, 256), F32),
        in_specs=[anywhere] * 3,
        out_specs=anywhere,
        scratch_shapes=[
            pltpu.VMEM((4, 24, 2, 32, 128), F32),
            pltpu.VMEM((3, 24, 2, 32, 128), F32),
            pltpu.VMEM((3, 24, 2, 32, 128), F32),
            pltpu.VMEM((3, 24, 2, 32, 128), F32),
            pltpu.VMEM((24, 2, 32, 128), F32),
            pltpu.VMEM((18, 2, 32, 128), F32),
            pltpu.VMEM((16, 2, 16, 128), F32),
            pltpu.VMEM((16, 2, 16, 128), F32),
            pltpu.VMEM((5, 2, 16, 2, 4, 128), F32),
            pltpu.VMEM((4, 2, 24, 2, 4, 128), F32),
            pltpu.VMEM((2, 16, 2, 1, 128), F32),
            pltpu.VMEM((2, 16, 2, 1, 128), F32),
            pltpu.VMEM((3, 8, 128), F32),
            pltpu.VMEM((32, 1, 128), F32),
            pltpu.VMEM((8, 1, 128), F32),
            pltpu.VMEM((2, 16, 16, 128), F32),
            pltpu.VMEM((2, 16, 16, 128), F32),
            dma((8,)), dma((3,)), dma((3,)), dma((4, 8)), dma((4, 8)),
            dma, dma, dma, dma, dma((2,)), dma((2,)), dma((2,)),
        ],
        compiler_params=pltpu.CompilerParams(collective_id=0, has_side_effects=True),
        cost_estimate=pl.CostEstimate(flops=50_000_000, bytes_accessed=3_000_000, transcendentals=0),
    )(init_field, source, damping)


def solution(mesh):
    block = P("gx", "yz", None)
    return jax.shard_map(
        per_device,
        mesh=mesh,
        in_specs=(block, block, block),
        out_specs=P("level", "gx", "yz", None),
        check_vma=False,
    )
```

```python
import functools

import jax
import jax.numpy as jnp
import numpy as np
from jax import lax
from jax.experimental import pallas as pl
from jax.experimental.pallas import tpu as pltpu
from jax.sharding import PartitionSpec as P

STEPS = 3
ITERS = 3
MESH = pl.DeviceIdType.MESH
F32 = jnp.float32

LOW, HIGH = 1.05, 15.0
MID, HALF = (LOW + HIGH) / 2, (HIGH - LOW) / 2
W = 6
LAST = 2 * W + 16
WINDOWS = ((1, (3, 11, 19, 21)), (2, (4, 12, 20)), (3, (5, 13, 19)), (4, (6, 14, 18)), (5, (7, 15, 17)))


def block_polynomial():
    cheb = np.polynomial.chebyshev
    low, high = 2.0, 13.5

    def third(lam):
        x = (lam - (low + high) / 2) / ((high - low) / 2)
        return 4 * x**3 - 3 * x

    nodes = np.cos(np.pi * (np.arange(4) + 0.5) / 4)
    lam = MID + HALF * nodes
    rho = cheb.chebfit(nodes, (1 + (lam - 1) * third(lam) / third(0.0)) / lam, 3)
    return [float(c) for c in cheb.chebmul(cheb.chebmul(rho, [0.0, 1.0]), [0.0, 0.0, 1.0])]


PSI = block_polynomial()


def planes(start, count, step, body):
    def turn(i, carry):
        for u in range(step):
            body(start + i * step + u)
        return carry

    lax.fori_loop(0, count // step, turn, 0)


def tree(terms):
    while len(terms) > 1:
        terms = [a + b for a, b in zip(terms[::2], terms[1::2])] + terms[len(terms) & ~1 :]
    return terms[0]


def zsum(v0, v1, first, last):
    a0, a1 = pltpu.roll(v0, 1, 1), pltpu.roll(v1, 1, 1)
    b0, b1 = pltpu.roll(v0, 127, 1), pltpu.roll(v1, 127, 1)
    n0 = jnp.where(first, 0.0, a0) + jnp.where(last, b1, b0)
    n1 = jnp.where(first, a0, a1) + jnp.where(last, 0.0, b1)
    return n0, n1


def recurrences(nu):
    def pattern(rows, values):
        j = lax.rem(lax.broadcasted_iota(jnp.int32, (rows, 128), 0), W)
        out = jnp.full((rows, 128), values[W - 1], F32)
        for q in range(W - 1):
            out = jnp.where(j == q, values[q], out)
        return out

    middle = W - 2
    bands = {1: (1.0,) + (0.5,) * middle + (0.5 / PSI[W],)}
    for o in range(-W + 1, 1):
        closing = -0.5 * PSI[W - 1 + o] / PSI[W] + (0.5 if o == -1 else 0.0)
        bands[o] = (0.0,) + ((0.5 if o == -1 else 0.0),) * middle + (closing,)
    long = {o: pattern(24, v) for o, v in bands.items()}
    short = {o: pattern(16, v) for o, v in bands.items()}

    def shifted(v, o):
        rows = v.shape[0]
        return v if o % rows == 0 else pltpu.roll(v, o % rows, 0)

    def times(z, shift):
        f, m = z
        fx = sum(shifted(f * short[o], o) for o in bands)
        mx = sum(long[o] * shifted(m, -o) for o in bands)
        return fx + shift * f, mx + shift * m

    def inner(y, z):
        return jnp.sum(y[0] * z[1][:16], axis=0, keepdims=True)

    def axpy(y, s, z):
        return y[0] + s * z[0], y[1] + s * z[1]

    one = jnp.where(lax.broadcasted_iota(jnp.int32, (16, 128), 0) == 0, 1.0, 0.0).astype(F32)
    start = (one, nu)

    def solve(resid, answer):
        direction = resid
        norm = inner(resid, resid)
        for step in range(ITERS):
            image = times(direction, MID / HALF)
            alpha = norm / inner(direction, image)
            answer = axpy(answer, alpha, direction) if answer else (alpha * direction[0], alpha * direction[1])
            if step + 1 < ITERS:
                resid = axpy(resid, -alpha, image)
                following = inner(resid, resid)
                direction = axpy(resid, following / norm, direction)
                norm = following
        return answer

    back = (MID - 1.0) / HALF
    states = [None]
    corrected = None
    for step in range(STEPS):
        state = states[-1]
        resid = axpy(start, -1.0, times(state, back)) if state else start
        states.append(solve(resid, state))
        change = axpy(states[-1], -1.0, state) if state else states[-1]
        inside = axpy(corrected, -0.5, change) if corrected else (-0.5 * change[0], -0.5 * change[1])
        resid = axpy(start, -1.0, times(inside, back))
        corrected = solve(resid, corrected)
    return states[-1][0] * (1.0 / HALF), corrected[0] * (1.0 / HALF)


def kernel(
    init_hbm, source_hbm, damping_hbm, out_hbm,
    u0, u1, u2, u3, u4, u5, diag, init, source, damping, ys, yr, ps, pr, sums, part_a, part_b, mine, theirs,
    local_sem, init_send, init_recv, ghost_send, ghost_recv,
    a_send, a_recv, b_send, b_recv, out_sem, out_send, out_recv,
):
    c = lax.axis_index("level")
    gx = lax.axis_index("gx")
    yz = lax.axis_index("yz")
    other = 1 - c
    beyond = lax.rem(gx + 2 * c + 3, 4)
    above, below = lax.rem(yz + 1, 32), lax.rem(yz + 31, 32)
    device_of = {
        "near": (other, gx, yz), "up": (c, gx, above), "down": (c, gx, below), "far": (other, beyond, yz),
        "near_up": (other, gx, above), "near_down": (other, gx, below),
        "far_up": (other, beyond, above), "far_down": (other, beyond, below),
    }
    y, z = lax.rem(yz, 4), lax.div(yz, 4)
    plane_slot = gx * 8 + c * 4 + y

    plane_mates = [
        (cc, xx, z * 4 + yy)
        for i, xx in enumerate([gx] + [lax.rem(gx + k, 4) for k in range(1, 4)])
        for j, cc in enumerate([c, other])
        for m, yy in enumerate([y] + [lax.rem(y + k, 4) for k in range(1, 4)])
        if i + j + m > 0
    ]
    line_mates = [(c, gx, lax.rem(z + k, 8) * 4 + y) for k in range(1, 8)]

    low_ok, high_ok = yz > 0, yz < 31
    x_low_ok, x_high_ok = gx + c > 0, gx + c < 4
    far_ok = jnp.logical_and(gx + 2 * c >= 1, gx + 2 * c <= 4)
    exists = {
        "near": None, "up": high_ok, "down": low_ok, "far": far_ok, "near_up": high_ok, "near_down": low_ok,
        "far_up": jnp.logical_and(far_ok, high_ok), "far_down": jnp.logical_and(far_ok, low_ok),
    }

    def where_there(name, act):
        if exists[name] is None:
            act()
        else:
            pl.when(exists[name])(act)
    barrier = pltpu.get_barrier_semaphore()

    def greet(device):
        pl.semaphore_signal(barrier, inc=1, device_id=device, device_id_type=MESH)

    for device in plane_mates:
        greet(device)
    greeted = 38
    own = pl.ds(c * 16, 16)
    rows = pl.ds(8, 16)
    loads = []
    for h in range(2):
        s = pl.ds(128 * h, 128)
        loads += [
            pltpu.make_async_copy(damping_hbm.at[own, :, s], damping.at[:, h], local_sem.at[h]),
            pltpu.make_async_copy(init_hbm.at[own, :, s], init.at[pl.ds(1, 16), h, rows], local_sem.at[2 + h]),
            pltpu.make_async_copy(
                init_hbm.at[pl.ds(16 - c, 1), :, s], init.at[pl.ds(17 - 17 * c, 1), h, rows], local_sem.at[4 + h]
            ),
            pltpu.make_async_copy(source_hbm.at[own, :, s], source.at[:, h], local_sem.at[6 + h]),
        ]
    for load in loads:
        load.start()

    for name, there in exists.items():
        where_there(
            name,
            functools.partial(greet, device_of[name]),
        )
        greeted = greeted + (1 if there is None else there.astype(jnp.int32))
    for device in line_mates:
        greet(device)

    lane = lax.broadcasted_iota(jnp.int32, (8, 128), 1)
    sublane = lax.broadcasted_iota(jnp.int32, (8, 128), 0)
    first, last = lane == 0, lane == 127
    has_low, has_high = low_ok.astype(F32), high_ok.astype(F32)
    x_low, x_high = x_low_ok.astype(F32), x_high_ok.astype(F32)

    def edge_of(x):
        return jnp.where(x < W, x_low, jnp.where(x >= W + 16, x_high, 1.0))

    def remote(src, dst, sends, recvs, name):
        return pltpu.make_async_remote_copy(
            src_ref=src, dst_ref=dst, send_sem=sends, recv_sem=recvs,
            device_id=device_of[name], device_id_type=MESH,
        )

    def exchange(e, ref):
        slab, into = ys.at[e], yr.at[e]
        step, top = 16 - W, 16 + W
        plan = (
            (slab.at[1], into.at[0, pl.ds(W, 16)], "up"),
            (slab.at[0], into.at[1, pl.ds(W, 16)], "down"),
            (ref.at[pl.ds(W + step * c, W), :, rows], ref.at[pl.ds(top - top * c, W), :, rows], "far"),
            (slab.at[1, pl.ds(11 * c, 5)], into.at[0, pl.ds(top - 21 * c, 5)], "far_up"),
            (slab.at[0, pl.ds(11 * c, 5)], into.at[1, pl.ds(top - 21 * c, 5)], "far_down"),
            (slab.at[1, pl.ds(11 - 11 * c, 5)], into.at[0, pl.ds(1 + 21 * c, 5)], "near_up"),
            (slab.at[0, pl.ds(11 - 11 * c, 5)], into.at[1, pl.ds(1 + 21 * c, 5)], "near_down"),
            (ref.at[pl.ds(16 - step * c, W), :, rows], ref.at[pl.ds(top * c, W), :, rows], "near"),
        )
        return [
            (name, remote(src, dst, ghost_send.at[e, i], ghost_recv.at[e, i], name))
            for i, (src, dst, name) in enumerate(plan)
        ]

    def launch(copies):
        for name, copy in copies:
            where_there(name, copy.start)

    def receive(copies):
        for name, copy in copies:
            turned = name.replace("up", "down") if "up" in name else name.replace("down", "up")
            where_there(turned, copy.wait_recv)

    def sent(copies):
        for name, copy in copies:
            where_there(name, copy.wait_send)

    def pack(e, t, x, h, tile):
        part = tile[0:6] if t == 0 else tile[2:8]
        if h == 0:
            ys[e, t, x, 0] = part[0:4]
            ys[e, t, x, 1, 0:2] = part[4:6]
        else:
            ys[e, t, x, 1, 2:4] = part[0:2]
            ys[e, t, x, 2] = part[2:6]

    for load in loads:
        load.wait()

    def prepare(x):
        for h in range(2):
            for t in range(2):
                at = pl.ds(8 * t, 8)
                d = (damping[x, h, at] + (7.0 - MID)) * (2.0 / HALF)
                diag[x + W, h, pl.ds(8 + 8 * t, 8)] = d
                pack(0, t, x, h, d)
            ps[0, x, h] = init[x + 1, h, 8:9]
            ps[1, x, h] = init[x + 1, h, 23:24]

    planes(0, 16, 8, prepare)
    pl.semaphore_wait(barrier, greeted)
    edges = [
        ("up", remote(ps.at[1], pr.at[0], init_send.at[0], init_recv.at[0], "up")),
        ("down", remote(ps.at[0], pr.at[1], init_send.at[1], init_recv.at[1], "down")),
        ("far", remote(
            init.at[pl.ds(1 + 15 * c, 1), :, rows], init.at[pl.ds(17 - 17 * c, 1), :, rows],
            init_send.at[2], init_recv.at[2], "far",
        )),
    ]
    launch(edges)
    launch(exchange(0, diag))
    receive(edges)
    for h in range(2):
        init[0, h, rows] = jnp.where(x_low_ok, init[0, h, rows], 0.0)
        init[17, h, rows] = jnp.where(x_high_ok, init[17, h, rows], 0.0)

    def neighbours_of(ref, x, at):
        v = [ref[x, h, pl.ds(at, 8)] for h in range(2)]
        n = zsum(*v, first, last)
        total = []
        for h in range(2):
            along_y = ref[x, h, pl.ds(at - 1, 8)] + ref[x, h, pl.ds(at + 1, 8)]
            total.append(n[h] + (along_y + (ref[x - 1, h, pl.ds(at, 8)] + ref[x + 1, h, pl.ds(at, 8)])))
        return v, total

    def edge_rows(x):
        for h in range(2):
            init[x + 1, h, 7:8] = jnp.where(low_ok, pr[0, x, h], 0.0)
            init[x + 1, h, 24:25] = jnp.where(high_ok, pr[1, x, h], 0.0)

    planes(0, 16, 16, edge_rows)

    def first_vector(x):
        for t in range(2):
            v, total = neighbours_of(init, x + 1, 8 + 8 * t)
            for h in range(2):
                at = pl.ds(8 * t, 8)
                w = source[x, h, at] - ((damping[x, h, at] + 6.0) * v[h] - total[h])
                u0[0, x + W, h, pl.ds(8 + 8 * t, 8)] = w
                pack(1, t, x, h, w)

    planes(0, 16, 16, first_vector)
    launch(exchange(1, u0.at[0]))

    def merge(e, ref):
        receive(exchange(e, ref))

        def ghosts(x):
            x_in = jnp.logical_and(jnp.logical_or(x >= W, x_low_ok), jnp.logical_or(x < W + 16, x_high_ok))
            for side, ok, at in ((0, low_ok, 2), (1, high_ok, 24)):
                there = jnp.logical_and(ok, x_in)
                group = [jnp.where(there, yr[e, side, x, g], 0.0) for g in range(3)]
                ref[x, 0, at : at + 4] = group[0]
                ref[x, 0, at + 4 : at + 6] = group[1][0:2]
                ref[x, 1, at : at + 2] = group[1][2:4]
                ref[x, 1, at + 2 : at + 6] = group[2]

        planes(0, LAST, 14, ghosts)
        for x in range(W):
            for h in range(2):
                ref[x, h, rows] = jnp.where(x_low_ok, ref[x, h, rows], 0.0)
                ref[W + 16 + x, h, rows] = jnp.where(x_high_ok, ref[W + 16 + x, h, rows], 0.0)

    merge(0, diag)

    def block_of(block, carry):
        basis = [u.at[block] for u in (u0, u1, u2, u3, u4, u5)]
        following = u0.at[block + 1]
        merge(block + 1, basis[0])
        for j, starts in WINDOWS:
            keep = []
            for at in starts:
                r = sublane + at
                keep.append(jnp.where(r < 8, has_low, jnp.where(r >= 24, has_high, 1.0)).astype(F32))

            def apply(x, j=j, starts=starts, keep=keep):
                edge = edge_of(x)
                for at, mask in zip(starts, keep):
                    v, total = neighbours_of(basis[j - 1], x, at)
                    for h in range(2):
                        t = diag[x, h, pl.ds(at, 8)] * v[h] - total[h] * (2.0 / HALF)
                        t = 0.5 * t if j == 1 else t - basis[j - 2][x, h, pl.ds(at, 8)]
                        basis[j][x, h, pl.ds(at, 8)] = t * (mask * edge)

            planes(j, LAST - 2 * j, LAST - 2 * j, apply)

        def close(i, carry):
            done = []
            for u in range(16):
                x = 16 * i + u + W
                for at in (8, 16):
                    v, total = neighbours_of(basis[W - 1], x, at)
                    for h in range(2):
                        old = [basis[q][x, h, pl.ds(at, 8)] for q in range(W - 1)]
                        new = diag[x, h, pl.ds(at, 8)] * v[h] - total[h] * (2.0 / HALF) - old[W - 2]
                        new = tree([PSI[W] * new] + [PSI[q] * f for q, f in enumerate(old + [v[h]])])
                        done.append((x, h, at, new))
            for x, h, at, new in done:
                following[x, h, pl.ds(at, 8)] = new
                t = at // 8 - 1
                pack(block + 2, t, x - W, h, new)
            return carry

        lax.fori_loop(0, 1, close, 0)

        @pl.when(block < 1)
        def _():
            launch(exchange(block + 2, following))

        def products(i, carry):
            gathered = [[] for _ in range(2 * W)]
            for u in range(4):
                for h in range(2):
                    for t in range(2):
                        v = [f[4 * i + u + W, h, pl.ds(8 + 8 * t, 8)] for f in (*basis, following)]
                        for q in range(W):
                            gathered[q].append(v[0] * v[q])
                            gathered[W + q].append(v[W] * v[q])
            return tuple(a + tree(terms) for a, terms in zip(carry, gathered))

        totals = lax.fori_loop(0, 4, products, (jnp.zeros((8, 128), F32),) * (2 * W))
        for q, total in enumerate(totals):
            sums[block, q : q + 1] = jnp.sum(total, axis=0, keepdims=True)
        return carry

    lax.fori_loop(0, 2, block_of, 0)

    diagonal = lax.broadcasted_iota(jnp.int32, (24, 128), 0) == lax.broadcasted_iota(jnp.int32, (24, 128), 1)

    def to_row(v):
        return jnp.sum(jnp.where(diagonal, v, 0.0), axis=0, keepdims=True)

    part_a[plane_slot] = to_row(jnp.sum(jnp.concatenate([sums[0, 0:12], sums[1, 0:12]], axis=0), axis=1, keepdims=True))

    def share(part, slot, sends, recvs, devices):
        for device in devices:
            pltpu.make_async_remote_copy(
                src_ref=part.at[slot], dst_ref=part.at[slot], send_sem=sends, recv_sem=recvs,
                device_id=device, device_id_type=MESH,
            ).start()

    def settle(part, sem):
        rest = part.at[pl.ds(0, part.shape[0] - 1)]
        pltpu.make_async_copy(rest, rest, sem).wait()

    share(part_a, plane_slot, a_send, a_recv, plane_mates)
    settle(part_a, a_recv)
    part_b[z] = jnp.sum(part_a[...], axis=0)
    share(part_b, z, b_send, b_recv, line_mates)
    settle(part_b, b_recv)
    total = jnp.sum(part_b[...], axis=0)
    nu = jnp.sum(jnp.where(diagonal, total, 0.0), axis=1, keepdims=True)
    predicted, corrected = recurrences(jnp.broadcast_to(nu, (24, 128)))

    upper = jnp.where(c == 1, 1.0, 0.0).astype(F32)
    away = [corrected[k : k + 1] + upper * (predicted[k : k + 1] - corrected[k : k + 1]) for k in range(12)]
    home = [predicted[k : k + 1] + upper * (corrected[k : k + 1] - predicted[k : k + 1]) for k in range(12)]

    away = [jnp.broadcast_to(w, (8, 128)) for w in away]
    home = [jnp.broadcast_to(w, (8, 128)) for w in home]

    def combine(ref, h, weights):
        def body(x):
            for t in range(2):
                at = pl.ds(8 + 8 * t, 8)
                terms = [weights[k] * (u0, u1, u2, u3, u4, u5)[k % W][k // W, x + W, h, at] for k in range(12)]
                ref[h, x, pl.ds(8 * t, 8)] = tree([init[x + 1, h, at]] + terms)

        planes(0, 16, 8, body)

    def place(h, part):
        return out_hbm.at[0, pl.ds(part * 16, 16), :, pl.ds(128 * h, 128)]

    gifts, keeps = [], []
    for h in range(2):
        combine(theirs, h, away)
        gifts.append(remote(theirs.at[h], place(h, c), out_send.at[h], out_recv.at[h], "near"))
        gifts[-1].start()
    for h in range(2):
        combine(mine, h, home)
        keeps.append(pltpu.make_async_copy(mine.at[h], place(h, c), out_sem.at[h]))
        keeps[-1].start()

    sent(edges)
    for e, ref in enumerate((diag, u0.at[0], u0.at[1])):
        sent(exchange(e, ref))
    for copy in gifts:
        copy.wait_send()

    settle(part_a, a_send)
    settle(part_b, b_send)
    for copy in keeps:
        copy.wait()
    for h in range(2):
        remote(theirs.at[h], place(h, other), out_send.at[h], out_recv.at[h], "near").wait_recv()


def per_device(init_field, source, damping):
    anywhere = pl.BlockSpec(memory_space=pl.ANY)
    dma = pltpu.SemaphoreType.DMA
    return pl.pallas_call(
        kernel,
        out_shape=jax.ShapeDtypeStruct((1, 32, 16, 256), F32),
        in_specs=[anywhere] * 3,
        out_specs=anywhere,
        scratch_shapes=[
            pltpu.VMEM((3, LAST, 2, 32, 128), F32),
            *[pltpu.VMEM((2, LAST, 2, 32, 128), F32)] * 5,
            pltpu.VMEM((LAST, 2, 32, 128), F32),
            pltpu.VMEM((18, 2, 32, 128), F32),
            pltpu.VMEM((16, 2, 16, 128), F32),
            pltpu.VMEM((16, 2, 16, 128), F32),
            pltpu.VMEM((4, 2, 16, 3, 4, 128), F32),
            pltpu.VMEM((3, 2, LAST, 3, 4, 128), F32),
            pltpu.VMEM((2, 16, 2, 1, 128), F32),
            pltpu.VMEM((2, 16, 2, 1, 128), F32),
            pltpu.VMEM((2, 16, 128), F32),
            pltpu.VMEM((32, 1, 128), F32),
            pltpu.VMEM((8, 1, 128), F32),
            pltpu.VMEM((2, 16, 16, 128), F32),
            pltpu.VMEM((2, 16, 16, 128), F32),
            dma((8,)), dma((3,)), dma((3,)), dma((3, 8)), dma((3, 8)),
            dma, dma, dma, dma, dma((2,)), dma((2,)), dma((2,)),
        ],
        compiler_params=pltpu.CompilerParams(collective_id=0, has_side_effects=True),
        cost_estimate=pl.CostEstimate(flops=50_000_000, bytes_accessed=3_000_000, transcendentals=0),
    )(init_field, source, damping)


def solution(mesh):
    block = P("gx", "yz", None)
    return jax.shard_map(
        per_device,
        mesh=mesh,
        in_specs=(block, block, block),
        out_specs=P("level", "gx", "yz", None),
        check_vma=False,
    )
```

```python
import functools

import jax
import jax.numpy as jnp
import numpy as np
from jax import lax
from jax.experimental import pallas as pl
from jax.experimental.pallas import tpu as pltpu
from jax.sharding import PartitionSpec as P

STEPS = 3
ITERS = 3
MESH = pl.DeviceIdType.MESH
F32 = jnp.float32

LOW, HIGH = 1.05, 15.0
MID, HALF = (LOW + HIGH) / 2, (HIGH - LOW) / 2
W = 6
LAST = 2 * W + 16
WINDOWS = ((1, (3, 11, 19, 21)), (2, (4, 12, 20)), (3, (5, 13, 19)), (4, (6, 14, 18)), (5, (7, 15, 17)))


def block_polynomial():
    cheb = np.polynomial.chebyshev
    low, high = 2.0, 13.5

    def third(lam):
        x = (lam - (low + high) / 2) / ((high - low) / 2)
        return 4 * x**3 - 3 * x

    nodes = np.cos(np.pi * (np.arange(4) + 0.5) / 4)
    lam = MID + HALF * nodes
    rho = cheb.chebfit(nodes, (1 + (lam - 1) * third(lam) / third(0.0)) / lam, 3)
    return [float(c) for c in cheb.chebmul(cheb.chebmul(rho, [0.0, 1.0]), [0.0, 0.0, 1.0])]


PSI = block_polynomial()


def planes(start, count, step, body):
    def turn(i, carry):
        for u in range(step):
            body(start + i * step + u)
        return carry

    lax.fori_loop(0, count // step, turn, 0)


def tree(terms):
    while len(terms) > 1:
        terms = [a + b for a, b in zip(terms[::2], terms[1::2])] + terms[len(terms) & ~1 :]
    return terms[0]


def zsum(v0, v1, first, last):
    a0, a1 = pltpu.roll(v0, 1, 1), pltpu.roll(v1, 1, 1)
    b0, b1 = pltpu.roll(v0, 127, 1), pltpu.roll(v1, 127, 1)
    n0 = jnp.where(first, 0.0, a0) + jnp.where(last, b1, b0)
    n1 = jnp.where(first, a0, a1) + jnp.where(last, 0.0, b1)
    return n0, n1


def recurrences(nu):
    def pattern(rows, values):
        j = lax.rem(lax.broadcasted_iota(jnp.int32, (rows, 128), 0), W)
        out = jnp.full((rows, 128), values[W - 1], F32)
        for q in range(W - 1):
            out = jnp.where(j == q, values[q], out)
        return out

    middle = W - 2
    bands = {1: (1.0,) + (0.5,) * middle + (0.5 / PSI[W],)}
    for o in range(-W + 1, 1):
        closing = -0.5 * PSI[W - 1 + o] / PSI[W] + (0.5 if o == -1 else 0.0)
        bands[o] = (0.0,) + ((0.5 if o == -1 else 0.0),) * middle + (closing,)
    long = {o: pattern(24, v) for o, v in bands.items()}
    short = {o: pattern(16, v) for o, v in bands.items()}

    def shifted(v, o):
        rows = v.shape[0]
        return v if o % rows == 0 else pltpu.roll(v, o % rows, 0)

    def times(z, shift):
        f, m = z
        fx = sum(shifted(f * short[o], o) for o in bands)
        mx = sum(long[o] * shifted(m, -o) for o in bands)
        return fx + shift * f, mx + shift * m

    def inner(y, z):
        return jnp.sum(y[0] * z[1][:16], axis=0, keepdims=True)

    def axpy(y, s, z):
        return y[0] + s * z[0], y[1] + s * z[1]

    one = jnp.where(lax.broadcasted_iota(jnp.int32, (16, 128), 0) == 0, 1.0, 0.0).astype(F32)
    start = (one, nu)

    def solve(resid, answer):
        direction = resid
        norm = inner(resid, resid)
        for step in range(ITERS):
            image = times(direction, MID / HALF)
            alpha = norm / inner(direction, image)
            answer = axpy(answer, alpha, direction) if answer else (alpha * direction[0], alpha * direction[1])
            if step + 1 < ITERS:
                resid = axpy(resid, -alpha, image)
                following = inner(resid, resid)
                direction = axpy(resid, following / norm, direction)
                norm = following
        return answer

    back = (MID - 1.0) / HALF
    states = [None]
    corrected = None
    for step in range(STEPS):
        state = states[-1]
        resid = axpy(start, -1.0, times(state, back)) if state else start
        states.append(solve(resid, state))
        change = axpy(states[-1], -1.0, state) if state else states[-1]
        inside = axpy(corrected, -0.5, change) if corrected else (-0.5 * change[0], -0.5 * change[1])
        resid = axpy(start, -1.0, times(inside, back))
        corrected = solve(resid, corrected)
    return states[-1][0] * (1.0 / HALF), corrected[0] * (1.0 / HALF)


def kernel(
    init_hbm, source_hbm, damping_hbm, out_hbm,
    u0, u1, u2, u3, u4, u5, diag, init, source, damping, ys, yr, ps, pr, sums, part_a, part_b, mine, theirs,
    local_sem, init_send, init_recv, ghost_send, ghost_recv,
    a_send, a_recv, b_send, b_recv, out_sem, out_send, out_recv,
):
    c = lax.axis_index("level")
    gx = lax.axis_index("gx")
    yz = lax.axis_index("yz")
    other = 1 - c
    beyond = lax.rem(gx + 2 * c + 3, 4)
    above, below = lax.rem(yz + 1, 32), lax.rem(yz + 31, 32)
    device_of = {
        "near": (other, gx, yz), "up": (c, gx, above), "down": (c, gx, below), "far": (other, beyond, yz),
        "near_up": (other, gx, above), "near_down": (other, gx, below),
        "far_up": (other, beyond, above), "far_down": (other, beyond, below),
    }
    y, z = lax.rem(yz, 4), lax.div(yz, 4)
    plane_slot = gx * 8 + c * 4 + y

    plane_mates = [
        (cc, xx, z * 4 + yy)
        for i, xx in enumerate([gx] + [lax.rem(gx + k, 4) for k in range(1, 4)])
        for j, cc in enumerate([c, other])
        for m, yy in enumerate([y] + [lax.rem(y + k, 4) for k in range(1, 4)])
        if i + j + m > 0
    ]
    line_mates = [(c, gx, lax.rem(z + k, 8) * 4 + y) for k in range(1, 8)]

    low_ok, high_ok = yz > 0, yz < 31
    x_low_ok, x_high_ok = gx + c > 0, gx + c < 4
    far_ok = jnp.logical_and(gx + 2 * c >= 1, gx + 2 * c <= 4)
    exists = {
        "near": None, "up": high_ok, "down": low_ok, "far": far_ok, "near_up": high_ok, "near_down": low_ok,
        "far_up": jnp.logical_and(far_ok, high_ok), "far_down": jnp.logical_and(far_ok, low_ok),
    }

    def where_there(name, act):
        if exists[name] is None:
            act()
        else:
            pl.when(exists[name])(act)
    barrier = pltpu.get_barrier_semaphore()

    def greet(device):
        pl.semaphore_signal(barrier, inc=1, device_id=device, device_id_type=MESH)

    for device in plane_mates:
        greet(device)
    greeted = 38
    own = pl.ds(c * 16, 16)
    rows = pl.ds(8, 16)
    loads = []
    for h in range(2):
        s = pl.ds(128 * h, 128)
        loads += [
            pltpu.make_async_copy(damping_hbm.at[own, :, s], damping.at[:, h], local_sem.at[h]),
            pltpu.make_async_copy(init_hbm.at[own, :, s], init.at[pl.ds(1, 16), h, rows], local_sem.at[2 + h]),
            pltpu.make_async_copy(
                init_hbm.at[pl.ds(16 - c, 1), :, s], init.at[pl.ds(17 - 17 * c, 1), h, rows], local_sem.at[4 + h]
            ),
            pltpu.make_async_copy(source_hbm.at[own, :, s], source.at[:, h], local_sem.at[6 + h]),
        ]
    for load in loads:
        load.start()

    for name, there in exists.items():
        where_there(
            name,
            functools.partial(greet, device_of[name]),
        )
        greeted = greeted + (1 if there is None else there.astype(jnp.int32))
    for device in line_mates:
        greet(device)

    lane = lax.broadcasted_iota(jnp.int32, (8, 128), 1)
    sublane = lax.broadcasted_iota(jnp.int32, (8, 128), 0)
    first, last = lane == 0, lane == 127
    has_low, has_high = low_ok.astype(F32), high_ok.astype(F32)
    x_low, x_high = x_low_ok.astype(F32), x_high_ok.astype(F32)

    def edge_of(x):
        return jnp.where(x < W, x_low, jnp.where(x >= W + 16, x_high, 1.0))

    def remote(src, dst, sends, recvs, name):
        return pltpu.make_async_remote_copy(
            src_ref=src, dst_ref=dst, send_sem=sends, recv_sem=recvs,
            device_id=device_of[name], device_id_type=MESH,
        )

    def exchange(e, ref):
        slab, into = ys.at[e], yr.at[e]
        step, top = 16 - W, 16 + W
        plan = (
            (slab.at[1, pl.ds(11 * c, 5)], into.at[0, pl.ds(top - 21 * c, 5)], "far_up"),
            (slab.at[0, pl.ds(11 * c, 5)], into.at[1, pl.ds(top - 21 * c, 5)], "far_down"),
            (slab.at[1, pl.ds(11 - 11 * c, 5)], into.at[0, pl.ds(1 + 21 * c, 5)], "near_up"),
            (slab.at[0, pl.ds(11 - 11 * c, 5)], into.at[1, pl.ds(1 + 21 * c, 5)], "near_down"),
            (slab.at[1], into.at[0, pl.ds(W, 16)], "up"),
            (slab.at[0], into.at[1, pl.ds(W, 16)], "down"),
            (ref.at[pl.ds(W + step * c, W), :, rows], ref.at[pl.ds(top - top * c, W), :, rows], "far"),
            (ref.at[pl.ds(16 - step * c, W), :, rows], ref.at[pl.ds(top * c, W), :, rows], "near"),
        )
        return [
            (name, remote(src, dst, ghost_send.at[e, i], ghost_recv.at[e, i], name))
            for i, (src, dst, name) in enumerate(plan)
        ]

    def launch(copies):
        for name, copy in copies:
            where_there(name, copy.start)

    def receive(copies):
        for name, copy in copies:
            turned = name.replace("up", "down") if "up" in name else name.replace("down", "up")
            where_there(turned, copy.wait_recv)

    def sent(copies):
        for name, copy in copies:
            where_there(name, copy.wait_send)

    def pack(e, t, x, h, tile):
        part = tile[0:6] if t == 0 else tile[2:8]
        if h == 0:
            ys[e, t, x, 0] = part[0:4]
            ys[e, t, x, 1, 0:2] = part[4:6]
        else:
            ys[e, t, x, 1, 2:4] = part[0:2]
            ys[e, t, x, 2] = part[2:6]

    for load in loads:
        load.wait()

    def prepare(x):
        for h in range(2):
            for t in range(2):
                at = pl.ds(8 * t, 8)
                d = (damping[x, h, at] + (7.0 - MID)) * (2.0 / HALF)
                diag[x + W, h, pl.ds(8 + 8 * t, 8)] = d
                pack(0, t, x, h, d)
            ps[0, x, h] = init[x + 1, h, 8:9]
            ps[1, x, h] = init[x + 1, h, 23:24]

    planes(0, 16, 8, prepare)
    pl.semaphore_wait(barrier, greeted)
    edges = [
        ("up", remote(ps.at[1], pr.at[0], init_send.at[0], init_recv.at[0], "up")),
        ("down", remote(ps.at[0], pr.at[1], init_send.at[1], init_recv.at[1], "down")),
        ("far", remote(
            init.at[pl.ds(1 + 15 * c, 1), :, rows], init.at[pl.ds(17 - 17 * c, 1), :, rows],
            init_send.at[2], init_recv.at[2], "far",
        )),
    ]
    launch(edges)
    launch(exchange(0, diag))
    receive(edges)
    for h in range(2):
        init[0, h, rows] = jnp.where(x_low_ok, init[0, h, rows], 0.0)
        init[17, h, rows] = jnp.where(x_high_ok, init[17, h, rows], 0.0)

    def neighbours_of(ref, x, at):
        v = [ref[x, h, pl.ds(at, 8)] for h in range(2)]
        n = zsum(*v, first, last)
        total = []
        for h in range(2):
            along_y = ref[x, h, pl.ds(at - 1, 8)] + ref[x, h, pl.ds(at + 1, 8)]
            total.append(n[h] + (along_y + (ref[x - 1, h, pl.ds(at, 8)] + ref[x + 1, h, pl.ds(at, 8)])))
        return v, total

    def edge_rows(x):
        for h in range(2):
            init[x + 1, h, 7:8] = jnp.where(low_ok, pr[0, x, h], 0.0)
            init[x + 1, h, 24:25] = jnp.where(high_ok, pr[1, x, h], 0.0)

    planes(0, 16, 16, edge_rows)

    def first_vector(x):
        for t in range(2):
            v, total = neighbours_of(init, x + 1, 8 + 8 * t)
            for h in range(2):
                at = pl.ds(8 * t, 8)
                w = source[x, h, at] - ((damping[x, h, at] + 6.0) * v[h] - total[h])
                u0[0, x + W, h, pl.ds(8 + 8 * t, 8)] = w
                pack(1, t, x, h, w)

    planes(0, 16, 16, first_vector)
    launch(exchange(1, u0.at[0]))

    def merge(e, ref):
        receive(exchange(e, ref))

        def ghosts(x):
            x_in = jnp.logical_and(jnp.logical_or(x >= W, x_low_ok), jnp.logical_or(x < W + 16, x_high_ok))
            for side, ok, at in ((0, low_ok, 2), (1, high_ok, 24)):
                there = jnp.logical_and(ok, x_in)
                group = [jnp.where(there, yr[e, side, x, g], 0.0) for g in range(3)]
                ref[x, 0, at : at + 4] = group[0]
                ref[x, 0, at + 4 : at + 6] = group[1][0:2]
                ref[x, 1, at : at + 2] = group[1][2:4]
                ref[x, 1, at + 2 : at + 6] = group[2]

        planes(0, LAST, 14, ghosts)
        for x in range(W):
            for h in range(2):
                ref[x, h, rows] = jnp.where(x_low_ok, ref[x, h, rows], 0.0)
                ref[W + 16 + x, h, rows] = jnp.where(x_high_ok, ref[W + 16 + x, h, rows], 0.0)

    merge(0, diag)

    def block_of(block, carry):
        basis = [u.at[block] for u in (u0, u1, u2, u3, u4, u5)]
        following = u0.at[block + 1]
        merge(block + 1, basis[0])
        for j, starts in WINDOWS:
            keep = []
            for at in starts:
                r = sublane + at
                keep.append(jnp.where(r < 8, has_low, jnp.where(r >= 24, has_high, 1.0)).astype(F32))

            def apply(x, j=j, starts=starts, keep=keep):
                edge = edge_of(x)
                for at, mask in zip(starts, keep):
                    v, total = neighbours_of(basis[j - 1], x, at)
                    for h in range(2):
                        t = diag[x, h, pl.ds(at, 8)] * v[h] - total[h] * (2.0 / HALF)
                        t = 0.5 * t if j == 1 else t - basis[j - 2][x, h, pl.ds(at, 8)]
                        basis[j][x, h, pl.ds(at, 8)] = t * (mask * edge)

            planes(j, LAST - 2 * j, LAST - 2 * j, apply)

        def close(i, carry):
            done = []
            for u in range(16):
                x = 16 * i + u + W
                for at in (8, 16):
                    v, total = neighbours_of(basis[W - 1], x, at)
                    for h in range(2):
                        old = [basis[q][x, h, pl.ds(at, 8)] for q in range(W - 1)]
                        new = diag[x, h, pl.ds(at, 8)] * v[h] - total[h] * (2.0 / HALF) - old[W - 2]
                        new = tree([PSI[W] * new] + [PSI[q] * f for q, f in enumerate(old + [v[h]])])
                        done.append((x, h, at, new))
            for x, h, at, new in done:
                following[x, h, pl.ds(at, 8)] = new
                t = at // 8 - 1
                pack(block + 2, t, x - W, h, new)
            return carry

        lax.fori_loop(0, 1, close, 0)

        @pl.when(block < 1)
        def _():
            launch(exchange(block + 2, following))

        def products(i, carry):
            gathered = [[] for _ in range(2 * W)]
            for u in range(4):
                for h in range(2):
                    for t in range(2):
                        v = [f[4 * i + u + W, h, pl.ds(8 + 8 * t, 8)] for f in (*basis, following)]
                        for q in range(W):
                            gathered[q].append(v[0] * v[q])
                            gathered[W + q].append(v[W] * v[q])
            return tuple(a + tree(terms) for a, terms in zip(carry, gathered))

        totals = lax.fori_loop(0, 4, products, (jnp.zeros((8, 128), F32),) * (2 * W))
        for q, total in enumerate(totals):
            sums[block, q : q + 1] = jnp.sum(total, axis=0, keepdims=True)
        return carry

    lax.fori_loop(0, 2, block_of, 0)

    diagonal = lax.broadcasted_iota(jnp.int32, (24, 128), 0) == lax.broadcasted_iota(jnp.int32, (24, 128), 1)

    def to_row(v):
        return jnp.sum(jnp.where(diagonal, v, 0.0), axis=0, keepdims=True)

    part_a[plane_slot] = to_row(jnp.sum(jnp.concatenate([sums[0, 0:12], sums[1, 0:12]], axis=0), axis=1, keepdims=True))

    def share(part, slot, sends, recvs, devices):
        for device in devices:
            pltpu.make_async_remote_copy(
                src_ref=part.at[slot], dst_ref=part.at[slot], send_sem=sends, recv_sem=recvs,
                device_id=device, device_id_type=MESH,
            ).start()

    def settle(part, sem):
        rest = part.at[pl.ds(0, part.shape[0] - 1)]
        pltpu.make_async_copy(rest, rest, sem).wait()

    share(part_a, plane_slot, a_send, a_recv, plane_mates)
    settle(part_a, a_recv)
    part_b[z] = jnp.sum(part_a[...], axis=0)
    share(part_b, z, b_send, b_recv, line_mates)
    settle(part_b, b_recv)
    total = jnp.sum(part_b[...], axis=0)
    nu = jnp.sum(jnp.where(diagonal, total, 0.0), axis=1, keepdims=True)
    predicted, corrected = recurrences(jnp.broadcast_to(nu, (24, 128)))

    upper = jnp.where(c == 1, 1.0, 0.0).astype(F32)
    away = [corrected[k : k + 1] + upper * (predicted[k : k + 1] - corrected[k : k + 1]) for k in range(12)]
    home = [predicted[k : k + 1] + upper * (corrected[k : k + 1] - predicted[k : k + 1]) for k in range(12)]

    away = [jnp.broadcast_to(w, (8, 128)) for w in away]
    home = [jnp.broadcast_to(w, (8, 128)) for w in home]

    def combine(ref, h, weights):
        def body(x):
            for t in range(2):
                at = pl.ds(8 + 8 * t, 8)
                terms = [weights[k] * (u0, u1, u2, u3, u4, u5)[k % W][k // W, x + W, h, at] for k in range(12)]
                ref[h, x, pl.ds(8 * t, 8)] = tree([init[x + 1, h, at]] + terms)

        planes(0, 16, 8, body)

    def place(h, part):
        return out_hbm.at[0, pl.ds(part * 16, 16), :, pl.ds(128 * h, 128)]

    gifts, keeps = [], []
    for h in range(2):
        combine(theirs, h, away)
        gifts.append(remote(theirs.at[h], place(h, c), out_send.at[h], out_recv.at[h], "near"))
        gifts[-1].start()
    for h in range(2):
        combine(mine, h, home)
        keeps.append(pltpu.make_async_copy(mine.at[h], place(h, c), out_sem.at[h]))
        keeps[-1].start()

    sent(edges)
    for e, ref in enumerate((diag, u0.at[0], u0.at[1])):
        sent(exchange(e, ref))
    for copy in gifts:
        copy.wait_send()

    settle(part_a, a_send)
    settle(part_b, b_send)
    for copy in keeps:
        copy.wait()
    for h in range(2):
        remote(theirs.at[h], place(h, other), out_send.at[h], out_recv.at[h], "near").wait_recv()


def per_device(init_field, source, damping):
    anywhere = pl.BlockSpec(memory_space=pl.ANY)
    dma = pltpu.SemaphoreType.DMA
    return pl.pallas_call(
        kernel,
        out_shape=jax.ShapeDtypeStruct((1, 32, 16, 256), F32),
        in_specs=[anywhere] * 3,
        out_specs=anywhere,
        scratch_shapes=[
            pltpu.VMEM((3, LAST, 2, 32, 128), F32),
            *[pltpu.VMEM((2, LAST, 2, 32, 128), F32)] * 5,
            pltpu.VMEM((LAST, 2, 32, 128), F32),
            pltpu.VMEM((18, 2, 32, 128), F32),
            pltpu.VMEM((16, 2, 16, 128), F32),
            pltpu.VMEM((16, 2, 16, 128), F32),
            pltpu.VMEM((4, 2, 16, 3, 4, 128), F32),
            pltpu.VMEM((3, 2, LAST, 3, 4, 128), F32),
            pltpu.VMEM((2, 16, 2, 1, 128), F32),
            pltpu.VMEM((2, 16, 2, 1, 128), F32),
            pltpu.VMEM((2, 16, 128), F32),
            pltpu.VMEM((32, 1, 128), F32),
            pltpu.VMEM((8, 1, 128), F32),
            pltpu.VMEM((2, 16, 16, 128), F32),
            pltpu.VMEM((2, 16, 16, 128), F32),
            dma((8,)), dma((3,)), dma((3,)), dma((3, 8)), dma((3, 8)),
            dma, dma, dma, dma, dma((2,)), dma((2,)), dma((2,)),
        ],
        compiler_params=pltpu.CompilerParams(collective_id=0, has_side_effects=True),
        cost_estimate=pl.CostEstimate(flops=50_000_000, bytes_accessed=3_000_000, transcendentals=0),
    )(init_field, source, damping)


def solution(mesh):
    block = P("gx", "yz", None)
    return jax.shard_map(
        per_device,
        mesh=mesh,
        in_specs=(block, block, block),
        out_specs=P("level", "gx", "yz", None),
        check_vma=False,
    )
```

```python
import functools

import jax
import jax.numpy as jnp
import numpy as np
from jax import lax
from jax.experimental import pallas as pl
from jax.experimental.pallas import tpu as pltpu
from jax.sharding import PartitionSpec as P

STEPS = 3
ITERS = 3
MESH = pl.DeviceIdType.MESH
F32 = jnp.float32

LOW, HIGH = 1.05, 15.0
MID, HALF = (LOW + HIGH) / 2, (HIGH - LOW) / 2
W = 6
LAST = 2 * W + 16
WINDOWS = ((1, (3, 11, 19, 21)), (2, (4, 12, 20)), (3, (5, 13, 19)), (4, (6, 14, 18)), (5, (7, 15, 17)))


def block_polynomial():
    cheb = np.polynomial.chebyshev
    low, high = 2.0, 13.5

    def third(lam):
        x = (lam - (low + high) / 2) / ((high - low) / 2)
        return 4 * x**3 - 3 * x

    nodes = np.cos(np.pi * (np.arange(4) + 0.5) / 4)
    lam = MID + HALF * nodes
    rho = cheb.chebfit(nodes, (1 + (lam - 1) * third(lam) / third(0.0)) / lam, 3)
    return [float(c) for c in cheb.chebmul(cheb.chebmul(rho, [0.0, 1.0]), [0.0, 0.0, 1.0])]


PSI = block_polynomial()


def planes(start, count, step, body):
    def turn(i, carry):
        for u in range(step):
            body(start + i * step + u)
        return carry

    lax.fori_loop(0, count // step, turn, 0)


def tree(terms):
    while len(terms) > 1:
        terms = [a + b for a, b in zip(terms[::2], terms[1::2])] + terms[len(terms) & ~1 :]
    return terms[0]


def zsum(v0, v1, first, last):
    a0, a1 = pltpu.roll(v0, 1, 1), pltpu.roll(v1, 1, 1)
    b0, b1 = pltpu.roll(v0, 127, 1), pltpu.roll(v1, 127, 1)
    n0 = jnp.where(first, 0.0, a0) + jnp.where(last, b1, b0)
    n1 = jnp.where(first, a0, a1) + jnp.where(last, 0.0, b1)
    return n0, n1


def recurrences(nu):
    def pattern(rows, values):
        j = lax.rem(lax.broadcasted_iota(jnp.int32, (rows, 128), 0), W)
        out = jnp.full((rows, 128), values[W - 1], F32)
        for q in range(W - 1):
            out = jnp.where(j == q, values[q], out)
        return out

    middle = W - 2
    bands = {1: (1.0,) + (0.5,) * middle + (0.5 / PSI[W],)}
    for o in range(-W + 1, 1):
        closing = -0.5 * PSI[W - 1 + o] / PSI[W] + (0.5 if o == -1 else 0.0)
        bands[o] = (0.0,) + ((0.5 if o == -1 else 0.0),) * middle + (closing,)
    long = {o: pattern(24, v) for o, v in bands.items()}
    short = {o: pattern(16, v) for o, v in bands.items()}

    def shifted(v, o):
        rows = v.shape[0]
        return v if o % rows == 0 else pltpu.roll(v, o % rows, 0)

    def times(z, shift):
        f, m = z
        fx = sum(shifted(f * short[o], o) for o in bands)
        mx = sum(long[o] * shifted(m, -o) for o in bands)
        return fx + shift * f, mx + shift * m

    def inner(y, z):
        return jnp.sum(y[0] * z[1][:16], axis=0, keepdims=True)

    def axpy(y, s, z):
        return y[0] + s * z[0], y[1] + s * z[1]

    one = jnp.where(lax.broadcasted_iota(jnp.int32, (16, 128), 0) == 0, 1.0, 0.0).astype(F32)
    start = (one, nu)

    def solve(resid, answer):
        direction = resid
        norm = inner(resid, resid)
        for step in range(ITERS):
            image = times(direction, MID / HALF)
            alpha = norm / inner(direction, image)
            answer = axpy(answer, alpha, direction) if answer else (alpha * direction[0], alpha * direction[1])
            if step + 1 < ITERS:
                resid = axpy(resid, -alpha, image)
                following = inner(resid, resid)
                direction = axpy(resid, following / norm, direction)
                norm = following
        return answer

    back = (MID - 1.0) / HALF
    states = [None]
    corrected = None
    for step in range(STEPS):
        state = states[-1]
        resid = axpy(start, -1.0, times(state, back)) if state else start
        states.append(solve(resid, state))
        change = axpy(states[-1], -1.0, state) if state else states[-1]
        inside = axpy(corrected, -0.5, change) if corrected else (-0.5 * change[0], -0.5 * change[1])
        resid = axpy(start, -1.0, times(inside, back))
        corrected = solve(resid, corrected)
    return states[-1][0] * (1.0 / HALF), corrected[0] * (1.0 / HALF)


def kernel(
    init_hbm, source_hbm, damping_hbm, out_hbm,
    u0, u1, u2, u3, u4, u5, diag, init, source, damping, ys, yr, ps, pr, sums, part_a, part_b, mine, theirs,
    local_sem, init_send, init_recv, ghost_send, ghost_recv,
    a_send, a_recv, b_send, b_recv, out_sem, out_send, out_recv,
):
    c = lax.axis_index("level")
    gx = lax.axis_index("gx")
    yz = lax.axis_index("yz")
    other = 1 - c
    beyond = lax.rem(gx + 2 * c + 3, 4)
    above, below = lax.rem(yz + 1, 32), lax.rem(yz + 31, 32)
    device_of = {
        "near": (other, gx, yz), "up": (c, gx, above), "down": (c, gx, below), "far": (other, beyond, yz),
        "near_up": (other, gx, above), "near_down": (other, gx, below),
        "far_up": (other, beyond, above), "far_down": (other, beyond, below),
    }
    y, z = lax.rem(yz, 4), lax.div(yz, 4)
    plane_slot = gx * 8 + c * 4 + y

    plane_mates = [
        (cc, xx, z * 4 + yy)
        for i, xx in enumerate([gx] + [lax.rem(gx + k, 4) for k in range(1, 4)])
        for j, cc in enumerate([c, other])
        for m, yy in enumerate([y] + [lax.rem(y + k, 4) for k in range(1, 4)])
        if i + j + m > 0
    ]
    line_mates = [(c, gx, lax.rem(z + k, 8) * 4 + y) for k in range(1, 8)]

    low_ok, high_ok = yz > 0, yz < 31
    x_low_ok, x_high_ok = gx + c > 0, gx + c < 4
    far_ok = jnp.logical_and(gx + 2 * c >= 1, gx + 2 * c <= 4)
    exists = {
        "near": None, "up": high_ok, "down": low_ok, "far": far_ok, "near_up": high_ok, "near_down": low_ok,
        "far_up": jnp.logical_and(far_ok, high_ok), "far_down": jnp.logical_and(far_ok, low_ok),
    }

    def where_there(name, act):
        if exists[name] is None:
            act()
        else:
            pl.when(exists[name])(act)
    barrier = pltpu.get_barrier_semaphore()

    def greet(device):
        pl.semaphore_signal(barrier, inc=1, device_id=device, device_id_type=MESH)

    for device in plane_mates:
        greet(device)
    greeted = 38
    own = pl.ds(c * 16, 16)
    rows = pl.ds(8, 16)
    loads = []
    for h in range(2):
        s = pl.ds(128 * h, 128)
        loads += [
            pltpu.make_async_copy(damping_hbm.at[own, :, s], damping.at[:, h], local_sem.at[h]),
            pltpu.make_async_copy(init_hbm.at[own, :, s], init.at[pl.ds(1, 16), h, rows], local_sem.at[2 + h]),
            pltpu.make_async_copy(
                init_hbm.at[pl.ds(16 - c, 1), :, s], init.at[pl.ds(17 - 17 * c, 1), h, rows], local_sem.at[4 + h]
            ),
            pltpu.make_async_copy(source_hbm.at[own, :, s], source.at[:, h], local_sem.at[6 + h]),
        ]
    for load in loads:
        load.start()

    for name, there in exists.items():
        where_there(
            name,
            functools.partial(greet, device_of[name]),
        )
        greeted = greeted + (1 if there is None else there.astype(jnp.int32))
    for device in line_mates:
        greet(device)

    lane = lax.broadcasted_iota(jnp.int32, (8, 128), 1)
    sublane = lax.broadcasted_iota(jnp.int32, (8, 128), 0)
    first, last = lane == 0, lane == 127
    has_low, has_high = low_ok.astype(F32), high_ok.astype(F32)
    x_low, x_high = x_low_ok.astype(F32), x_high_ok.astype(F32)

    def edge_of(x):
        return jnp.where(x < W, x_low, jnp.where(x >= W + 16, x_high, 1.0))

    def remote(src, dst, sends, recvs, name):
        return pltpu.make_async_remote_copy(
            src_ref=src, dst_ref=dst, send_sem=sends, recv_sem=recvs,
            device_id=device_of[name], device_id_type=MESH,
        )

    def exchange(e, ref):
        slab, into = ys.at[e], yr.at[e]
        step, top = 16 - W, 16 + W
        plan = (
            (slab.at[1, pl.ds(11 * c, 5)], into.at[0, pl.ds(top - 21 * c, 5)], "far_up"),
            (slab.at[0, pl.ds(11 * c, 5)], into.at[1, pl.ds(top - 21 * c, 5)], "far_down"),
            (slab.at[1, pl.ds(11 - 11 * c, 5)], into.at[0, pl.ds(1 + 21 * c, 5)], "near_up"),
            (slab.at[0, pl.ds(11 - 11 * c, 5)], into.at[1, pl.ds(1 + 21 * c, 5)], "near_down"),
            (slab.at[1], into.at[0, pl.ds(W, 16)], "up"),
            (slab.at[0], into.at[1, pl.ds(W, 16)], "down"),
            (ref.at[pl.ds(W + step * c, W), :, rows], ref.at[pl.ds(top - top * c, W), :, rows], "far"),
            (ref.at[pl.ds(16 - step * c, W), :, rows], ref.at[pl.ds(top * c, W), :, rows], "near"),
        )
        return [
            (name, remote(src, dst, ghost_send.at[e, i], ghost_recv.at[e, i], name))
            for i, (src, dst, name) in enumerate(plan)
        ]

    def launch(copies):
        for name, copy in copies:
            where_there(name, copy.start)

    def receive(copies):
        for name, copy in copies:
            turned = name.replace("up", "down") if "up" in name else name.replace("down", "up")
            where_there(turned, copy.wait_recv)

    def sent(copies):
        for name, copy in copies:
            where_there(name, copy.wait_send)

    def pack(e, t, x, h, tile):
        part = tile[0:6] if t == 0 else tile[2:8]
        if h == 0:
            ys[e, t, x, 0] = part[0:4]
            ys[e, t, x, 1, 0:2] = part[4:6]
        else:
            ys[e, t, x, 1, 2:4] = part[0:2]
            ys[e, t, x, 2] = part[2:6]

    for load in loads:
        load.wait()

    def prepare(x):
        for h in range(2):
            for t in range(2):
                at = pl.ds(8 * t, 8)
                d = (damping[x, h, at] + (7.0 - MID)) * (2.0 / HALF)
                diag[x + W, h, pl.ds(8 + 8 * t, 8)] = d
                pack(0, t, x, h, d)
            ps[0, x, h] = init[x + 1, h, 8:9]
            ps[1, x, h] = init[x + 1, h, 23:24]

    planes(0, 16, 8, prepare)
    pl.semaphore_wait(barrier, greeted)
    edges = [
        ("up", remote(ps.at[1], pr.at[0], init_send.at[0], init_recv.at[0], "up")),
        ("down", remote(ps.at[0], pr.at[1], init_send.at[1], init_recv.at[1], "down")),
        ("far", remote(
            init.at[pl.ds(1 + 15 * c, 1), :, rows], init.at[pl.ds(17 - 17 * c, 1), :, rows],
            init_send.at[2], init_recv.at[2], "far",
        )),
    ]
    launch(edges)
    launch(exchange(0, diag))
    receive(edges)
    for h in range(2):
        init[0, h, rows] = jnp.where(x_low_ok, init[0, h, rows], 0.0)
        init[17, h, rows] = jnp.where(x_high_ok, init[17, h, rows], 0.0)

    def neighbours_of(ref, x, at):
        v = [ref[x, h, pl.ds(at, 8)] for h in range(2)]
        n = zsum(*v, first, last)
        total = []
        for h in range(2):
            along_y = ref[x, h, pl.ds(at - 1, 8)] + ref[x, h, pl.ds(at + 1, 8)]
            total.append(n[h] + (along_y + (ref[x - 1, h, pl.ds(at, 8)] + ref[x + 1, h, pl.ds(at, 8)])))
        return v, total

    def edge_rows(x):
        for h in range(2):
            init[x + 1, h, 7:8] = jnp.where(low_ok, pr[0, x, h], 0.0)
            init[x + 1, h, 24:25] = jnp.where(high_ok, pr[1, x, h], 0.0)

    planes(0, 16, 16, edge_rows)

    def first_vector(x):
        for t in range(2):
            v, total = neighbours_of(init, x + 1, 8 + 8 * t)
            for h in range(2):
                at = pl.ds(8 * t, 8)
                w = source[x, h, at] - ((damping[x, h, at] + 6.0) * v[h] - total[h])
                u0[0, x + W, h, pl.ds(8 + 8 * t, 8)] = w
                pack(1, t, x, h, w)

    planes(0, 16, 16, first_vector)
    launch(exchange(1, u0.at[0]))

    def merge(e, ref):
        receive(exchange(e, ref))

        def ghosts(x):
            x_in = jnp.logical_and(jnp.logical_or(x >= W, x_low_ok), jnp.logical_or(x < W + 16, x_high_ok))
            for side, ok, at in ((0, low_ok, 2), (1, high_ok, 24)):
                there = jnp.logical_and(ok, x_in)
                group = [jnp.where(there, yr[e, side, x, g], 0.0) for g in range(3)]
                ref[x, 0, at : at + 4] = group[0]
                ref[x, 0, at + 4 : at + 6] = group[1][0:2]
                ref[x, 1, at : at + 2] = group[1][2:4]
                ref[x, 1, at + 2 : at + 6] = group[2]

        planes(0, LAST, 14, ghosts)
        for x in range(W):
            for h in range(2):
                ref[x, h, rows] = jnp.where(x_low_ok, ref[x, h, rows], 0.0)
                ref[W + 16 + x, h, rows] = jnp.where(x_high_ok, ref[W + 16 + x, h, rows], 0.0)

    merge(0, diag)

    def block_of(block, carry):
        basis = [u.at[block] for u in (u0, u1, u2, u3, u4, u5)]
        following = u0.at[block + 1]
        merge(block + 1, basis[0])
        for j, starts in WINDOWS:
            keep = []
            for at in starts:
                r = sublane + at
                keep.append(jnp.where(r < 8, has_low, jnp.where(r >= 24, has_high, 1.0)).astype(F32))

            def apply(x, j=j, starts=starts, keep=keep):
                edge = edge_of(x)
                for at, mask in zip(starts, keep):
                    v, total = neighbours_of(basis[j - 1], x, at)
                    for h in range(2):
                        t = diag[x, h, pl.ds(at, 8)] * v[h] - total[h] * (2.0 / HALF)
                        t = 0.5 * t if j == 1 else t - basis[j - 2][x, h, pl.ds(at, 8)]
                        basis[j][x, h, pl.ds(at, 8)] = t * (mask * edge)

            planes(j, LAST - 2 * j, LAST - 2 * j, apply)

        def close(i, carry):
            done = []
            for u in range(16):
                x = 16 * i + u + W
                for at in (8, 16):
                    v, total = neighbours_of(basis[W - 1], x, at)
                    for h in range(2):
                        old = [basis[q][x, h, pl.ds(at, 8)] for q in range(W - 1)]
                        new = diag[x, h, pl.ds(at, 8)] * v[h] - total[h] * (2.0 / HALF) - old[W - 2]
                        new = tree([PSI[W] * new] + [PSI[q] * f for q, f in enumerate(old + [v[h]])])
                        done.append((x, h, at, new))
            for x, h, at, new in done:
                following[x, h, pl.ds(at, 8)] = new
                t = at // 8 - 1
                pack(block + 2, t, x - W, h, new)
            return carry

        lax.fori_loop(0, 1, close, 0)

        @pl.when(block < 1)
        def _():
            launch(exchange(block + 2, following))

        def products(i, carry):
            for part in range(4):
                gathered = [[] for _ in range(2 * W)]
                for u in range(2):
                    for h in range(2):
                        for t in range(2):
                            x = 8 * i + 2 * part + u + W
                            v = [f[x, h, pl.ds(8 + 8 * t, 8)] for f in (*basis, following)]
                            for q in range(W):
                                gathered[q].append(v[0] * v[q])
                                gathered[W + q].append(v[W] * v[q])
                carry = tuple(a + tree(terms) for a, terms in zip(carry, gathered))
            return carry

        totals = lax.fori_loop(0, 2, products, (jnp.zeros((8, 128), F32),) * (2 * W))
        for q, total in enumerate(totals):
            sums[block, q : q + 1] = jnp.sum(total, axis=0, keepdims=True)
        return carry

    lax.fori_loop(0, 2, block_of, 0)

    diagonal = lax.broadcasted_iota(jnp.int32, (24, 128), 0) == lax.broadcasted_iota(jnp.int32, (24, 128), 1)

    def to_row(v):
        return jnp.sum(jnp.where(diagonal, v, 0.0), axis=0, keepdims=True)

    part_a[plane_slot] = to_row(jnp.sum(jnp.concatenate([sums[0, 0:12], sums[1, 0:12]], axis=0), axis=1, keepdims=True))

    def share(part, slot, sends, recvs, devices):
        for device in devices:
            pltpu.make_async_remote_copy(
                src_ref=part.at[slot], dst_ref=part.at[slot], send_sem=sends, recv_sem=recvs,
                device_id=device, device_id_type=MESH,
            ).start()

    def settle(part, sem):
        rest = part.at[pl.ds(0, part.shape[0] - 1)]
        pltpu.make_async_copy(rest, rest, sem).wait()

    share(part_a, plane_slot, a_send, a_recv, plane_mates)
    settle(part_a, a_recv)
    part_b[z] = jnp.sum(part_a[...], axis=0)
    share(part_b, z, b_send, b_recv, line_mates)
    settle(part_b, b_recv)
    total = jnp.sum(part_b[...], axis=0)
    nu = jnp.sum(jnp.where(diagonal, total, 0.0), axis=1, keepdims=True)
    predicted, corrected = recurrences(jnp.broadcast_to(nu, (24, 128)))

    upper = jnp.where(c == 1, 1.0, 0.0).astype(F32)
    away = [corrected[k : k + 1] + upper * (predicted[k : k + 1] - corrected[k : k + 1]) for k in range(12)]
    home = [predicted[k : k + 1] + upper * (corrected[k : k + 1] - predicted[k : k + 1]) for k in range(12)]

    away = [jnp.broadcast_to(w, (8, 128)) for w in away]
    home = [jnp.broadcast_to(w, (8, 128)) for w in home]

    def combine(ref, h, weights):
        def body(x):
            for t in range(2):
                at = pl.ds(8 + 8 * t, 8)
                terms = [weights[k] * (u0, u1, u2, u3, u4, u5)[k % W][k // W, x + W, h, at] for k in range(12)]
                ref[h, x, pl.ds(8 * t, 8)] = tree([init[x + 1, h, at]] + terms)

        planes(0, 16, 8, body)

    def place(h, part):
        return out_hbm.at[0, pl.ds(part * 16, 16), :, pl.ds(128 * h, 128)]

    gifts, keeps = [], []
    for h in range(2):
        combine(theirs, h, away)
        gifts.append(remote(theirs.at[h], place(h, c), out_send.at[h], out_recv.at[h], "near"))
        gifts[-1].start()
    for h in range(2):
        combine(mine, h, home)
        keeps.append(pltpu.make_async_copy(mine.at[h], place(h, c), out_sem.at[h]))
        keeps[-1].start()

    sent(edges)
    for e, ref in enumerate((diag, u0.at[0], u0.at[1])):
        sent(exchange(e, ref))
    for copy in gifts:
        copy.wait_send()

    settle(part_a, a_send)
    settle(part_b, b_send)
    for copy in keeps:
        copy.wait()
    for h in range(2):
        remote(theirs.at[h], place(h, other), out_send.at[h], out_recv.at[h], "near").wait_recv()


def per_device(init_field, source, damping):
    anywhere = pl.BlockSpec(memory_space=pl.ANY)
    dma = pltpu.SemaphoreType.DMA
    return pl.pallas_call(
        kernel,
        out_shape=jax.ShapeDtypeStruct((1, 32, 16, 256), F32),
        in_specs=[anywhere] * 3,
        out_specs=anywhere,
        scratch_shapes=[
            pltpu.VMEM((3, LAST, 2, 32, 128), F32),
            *[pltpu.VMEM((2, LAST, 2, 32, 128), F32)] * 5,
            pltpu.VMEM((LAST, 2, 32, 128), F32),
            pltpu.VMEM((18, 2, 32, 128), F32),
            pltpu.VMEM((16, 2, 16, 128), F32),
            pltpu.VMEM((16, 2, 16, 128), F32),
            pltpu.VMEM((4, 2, 16, 3, 4, 128), F32),
            pltpu.VMEM((3, 2, LAST, 3, 4, 128), F32),
            pltpu.VMEM((2, 16, 2, 1, 128), F32),
            pltpu.VMEM((2, 16, 2, 1, 128), F32),
            pltpu.VMEM((2, 16, 128), F32),
            pltpu.VMEM((32, 1, 128), F32),
            pltpu.VMEM((8, 1, 128), F32),
            pltpu.VMEM((2, 16, 16, 128), F32),
            pltpu.VMEM((2, 16, 16, 128), F32),
            dma((8,)), dma((3,)), dma((3,)), dma((3, 8)), dma((3, 8)),
            dma, dma, dma, dma, dma((2,)), dma((2,)), dma((2,)),
        ],
        compiler_params=pltpu.CompilerParams(collective_id=0, has_side_effects=True),
        cost_estimate=pl.CostEstimate(flops=50_000_000, bytes_accessed=3_000_000, transcendentals=0),
    )(init_field, source, damping)


def solution(mesh):
    block = P("gx", "yz", None)
    return jax.shard_map(
        per_device,
        mesh=mesh,
        in_specs=(block, block, block),
        out_specs=P("level", "gx", "yz", None),
        check_vma=False,
    )
```
